8 devices in a mesh: data: 8 (over z, y, x, core).
Axes of the slice: x: 2, y: 2, z: 1, core: 2. Of those that a mesh axis runs over, the one named last changes fastest.
Arguments:
- view_one: bfloat16 [1024, 256], P('data')
- view_two: bfloat16 [1024, 256], P('data')
- protos: bfloat16 [16384, 256], replicated
- valid_mask: int32 [1024], P('data')
Outputs:
- output 1: float32 [1024, 16384], P('data')
- output 2: float32 [1024, 16384], P('data')
- output 3: float32 [], replicated
- output 4: float32 [1024, 256], P('data')
- output 5: float32 [1024, 256], P('data')
- output 6: float32 [16384, 256], replicated
All inputs are finite; a program needn't handle non-finite values.
Results may differ from the reference program's by a relative error of at most 0.001.
Values are sent between devices in bfloat16 or wider.
A program may use at most 1 GiB of HBM per device.

```python
import jax
import jax.numpy as jnp

ROWS_DEV = 128
GROUPS = 8
PROTOS = 16384
EMBED_DIM = 256
SINK_ITERS = 3
SINK_EPS = 0.05
SOFT_TEMP = 0.1


def unit_rows(matrix):
    return matrix / jnp.sqrt(jnp.sum(matrix * matrix, axis=1, keepdims=True))


def draw_mask(draw_key):
    count_key, order_key = jax.random.split(draw_key)
    counts = jax.random.randint(count_key, (GROUPS,), 1, ROWS_DEV + 1)
    counts = counts.at[0].set(ROWS_DEV).at[1].set(1)
    order_scores = jax.random.randint(order_key, (GROUPS, ROWS_DEV), 0, 1 << 20) * ROWS_DEV + jnp.arange(ROWS_DEV, dtype=jnp.int32)[None, :]
    row_ranks = jnp.argsort(jnp.argsort(order_scores, axis=1), axis=1)
    return (row_ranks < counts[:, None]).astype(jnp.int32).reshape(-1)


def draw_picks(draw_key):
    band_width = max(2 * PROTOS // GROUPS, 1)
    starts = jnp.arange(GROUPS, dtype=jnp.int32)[:, None] * (PROTOS // GROUPS)
    offsets = jax.random.randint(draw_key, (GROUPS, ROWS_DEV), 0, band_width)
    return ((starts + offsets) % PROTOS).reshape(-1)


def draw_view(draw_key, protos, pick_ids):
    noise_rows = jax.random.normal(draw_key, (GROUPS * ROWS_DEV, EMBED_DIM), jnp.float32) * EMBED_DIM ** -0.5
    return unit_rows(0.6 * protos[pick_ids] + 0.8 * noise_rows)


def setup_inputs(seed: int = 0) -> dict:
    root_key = jax.random.key(seed)
    proto_key, pick_key, one_key, two_key, mask_key = jax.random.split(root_key, 5)
    protos = unit_rows(jax.random.normal(proto_key, (PROTOS, EMBED_DIM), jnp.float32))
    pick_ids = draw_picks(pick_key)
    return {
        "view_one": draw_view(one_key, protos, pick_ids).astype(jnp.bfloat16),
        "view_two": draw_view(two_key, protos, pick_ids).astype(jnp.bfloat16),
        "protos": protos.astype(jnp.bfloat16),
        "valid_mask": draw_mask(mask_key),
    }


def sinkhorn_codes(scores, weights, valid_count):
    transport = jnp.exp(scores / SINK_EPS) * weights
    for sweep_idx in range(SINK_ITERS):
        col_sum = jnp.sum(transport, axis=0, keepdims=True)
        transport = transport / (PROTOS * col_sum)
        row_sum = jnp.sum(transport, axis=1, keepdims=True) + (1.0 - weights)
        transport = transport / (valid_count * row_sum)
    return transport * valid_count


def reference(view_one, view_two, protos, valid_mask):
    weights = valid_mask.astype(jnp.float32)[:, None]
    valid_count = jnp.sum(weights)
    score_one = jnp.dot(view_one, protos.T, preferred_element_type=jnp.float32)
    score_two = jnp.dot(view_two, protos.T, preferred_element_type=jnp.float32)
    codes_one = sinkhorn_codes(score_one, weights, valid_count)
    codes_two = sinkhorn_codes(score_two, weights, valid_count)
    logp_one = jax.nn.log_softmax(score_one / SOFT_TEMP, axis=1)
    logp_two = jax.nn.log_softmax(score_two / SOFT_TEMP, axis=1)
    loss_value = -(jnp.sum(codes_two * logp_one) + jnp.sum(codes_one * logp_two)) / (2.0 * valid_count)
    grad_scale = weights / (2.0 * valid_count * SOFT_TEMP)
    grad_one = ((jnp.exp(logp_one) - codes_two) * grad_scale).astype(jnp.bfloat16)
    grad_two = ((jnp.exp(logp_two) - codes_one) * grad_scale).astype(jnp.bfloat16)
    dz_one = jnp.dot(grad_one, protos, preferred_element_type=jnp.float32)
    dz_two = jnp.dot(grad_two, protos, preferred_element_type=jnp.float32)
    d_protos = (jnp.dot(grad_one.T, view_one, preferred_element_type=jnp.float32)
                + jnp.dot(grad_two.T, view_two, preferred_element_type=jnp.float32))
    return codes_one, codes_two, loss_value, dz_one, dz_two, d_protos
```

```python
import functools

import jax
import jax.numpy as jnp
from jax import lax
from jax.experimental import pallas as pl
from jax.experimental.pallas import tpu as pltpu
from jax.sharding import PartitionSpec as P

SOFT_TEMP = 0.1
LOG2E = 1.4426950408889634
C_EXP = LOG2E / SOFT_TEMP
MESH = pl.DeviceIdType.MESH
NDEV = 8
ROWS = 128
NS = NDEV * ROWS
DIM = 256
KALL = 16384
KLOC = KALL // NDEV
GRP = 32
TK = 2048
SUB = 512
NT = 256

NT_DIMS = (((1,), (1,)), ((), ()))


def dot_nt(x, y):
    return lax.dot_general(x, y, NT_DIMS, preferred_element_type=jnp.float32)


def dot_nn(x, y):
    return jnp.dot(x, y, preferred_element_type=jnp.float32)


def sink_kernel(z1_ref, z2_ref, m_ref, c_hbm,
                zc1_ref, zc2_ref, vecs_ref, own_ref, b_out, meta_ref, stat_ref,
                z_all, m_all, cs, ps, s_ref, e_ref, bcol, ar1, ar2, ar3, b_all,
                c_sem, loc_sem, m_send, m_recv, z_send, z_recv, f_send, f_recv,
                ar_send, ar_recv, b_send, b_recv):
    me = lax.axis_index("data")
    chip, core = me // 2, me % 2
    partner = 2 * chip + (1 - core)
    peers = [lax.rem(me + o, NDEV) for o in range(1, NDEV)]
    same = [2 * lax.rem(chip + d, 4) + core for d in range(1, 4)]

    cslice = pltpu.make_async_copy(c_hbm.at[pl.ds(me * KLOC, KLOC), :], cs, c_sem)
    cslice.start()
    m_all[me] = jnp.broadcast_to(m_ref[...].astype(jnp.float32), (8, ROWS))
    z_all[0, me] = z1_ref[...]
    z_all[1, me] = z2_ref[...]

    barrier = pltpu.get_barrier_semaphore()
    for peer in peers:
        pl.semaphore_signal(barrier, inc=1, device_id=(peer,), device_id_type=MESH)
    pl.semaphore_wait(barrier, NDEV - 1)

    m_copies = []
    for o, peer in enumerate(peers):
        cp = pltpu.make_async_remote_copy(
            src_ref=m_all.at[me], dst_ref=m_all.at[me], send_sem=m_send.at[o],
            recv_sem=m_recv.at[o], device_id=(peer,), device_id_type=MESH)
        cp.start()
        m_copies.append(cp)
    z_copies = []
    for v, src in enumerate((z1_ref, z2_ref)):
        row = []
        for d, peer in enumerate(same + [partner]):
            cp = pltpu.make_async_remote_copy(
                src_ref=src, dst_ref=z_all.at[v, me], send_sem=z_send.at[v, d],
                recv_sem=z_recv.at[v, d], device_id=(peer,), device_id_type=MESH)
            cp.start()
            row.append(cp)
        z_copies.append(row)

    for cp in m_copies:
        cp.wait_recv()

    tri = (lax.broadcasted_iota(jnp.int32, (ROWS, ROWS), 0)
           < lax.broadcasted_iota(jnp.int32, (ROWS, ROWS), 1)).astype(jnp.bfloat16)
    base = jnp.zeros((8, 1), jnp.float32)
    pos_list = []
    for d in range(NDEV):
        md = m_all[d]
        pre = dot_nn(md.astype(jnp.bfloat16), tri) + base
        pos_list.append(jnp.where(md > 0, pre, -1.0))
        base = base + jnp.sum(md, axis=1, keepdims=True)
    pos = jnp.concatenate(pos_list, axis=1)
    count = base
    mask = (lax.broadcasted_iota(jnp.int32, (8, NS), 1).astype(jnp.float32) < count)
    maskf = mask.astype(jnp.float32)
    for t in range(NS // 128):
        idx = (lax.broadcasted_iota(jnp.int32, (128, NS), 0) + t * 128).astype(jnp.float32)
        ps[t * 128:(t + 1) * 128, :] = (jnp.broadcast_to(pos[0:1], (128, NS)) == idx).astype(jnp.bfloat16)

    fwd = []
    for v in range(2):
        for d in range(3):
            z_copies[v][d].wait_recv()
            frm = 2 * lax.rem(chip + 3 - d, 4) + core
            cp = pltpu.make_async_remote_copy(
                src_ref=z_all.at[v, frm], dst_ref=z_all.at[v, frm], send_sem=f_send.at[v, d],
                recv_sem=f_recv.at[v, d], device_id=(partner,), device_id_type=MESH)
            cp.start()
            fwd.append(cp)

    cslice.wait()
    for v, zc_ref in enumerate((zc1_ref, zc2_ref)):
        z_copies[v][3].wait_recv()
        for d in range(3):
            fwd[3 * v + d].wait_recv()
        zv = z_all[v].reshape(NS, DIM)
        for t in range(NS // 256):
            rows = slice(t * 256, (t + 1) * 256)
            zc_ref[rows, :] = dot_nn(ps[rows, :], zv).astype(jnp.bfloat16)

    CH = GRP * 8
    nch = KLOC // CH

    def first_pass(v, zc_ref):
        def body(i, carry):
            racc, lacc = carry
            off = pl.multiple_of(i * CH, CH)
            s_ref[v, pl.ds(off, CH), :] = dot_nt(cs[pl.ds(off, CH), :], zc_ref[...])
            for g in range(GRP):
                rows = pl.ds(off + g * 8, 8)
                p = jnp.exp2(s_ref[v, rows, :] * C_EXP)
                lacc = lacc + p
                e = p * p * maskf
                e_ref[v, rows, :] = e
                b = 1.0 / jnp.sum(e, axis=1, keepdims=True)
                racc = racc + e * b
            return racc, lacc
        zero = jnp.zeros((8, NS), jnp.float32)
        return lax.fori_loop(0, nch, body, (zero, zero))

    def exchange(idx, buf):
        copies = []
        for o, peer in enumerate(peers):
            cp = pltpu.make_async_remote_copy(
                src_ref=buf.at[me], dst_ref=buf.at[me], send_sem=ar_send.at[idx, o],
                recv_sem=ar_recv.at[idx, o], device_id=(peer,), device_id_type=MESH)
            cp.start()
            copies.append(cp)
        return copies

    def total(buf):
        acc = buf[0]
        for d in range(1, NDEV):
            acc = acc + buf[d]
        return acc

    def rsum(x):
        return jnp.sum(x, axis=0, keepdims=True)

    for v, zc_ref in enumerate((zc1_ref, zc2_ref)):
        racc, lacc = first_pass(v, zc_ref)
        ar1[me, v:v + 1, :] = rsum(racc)
        ar1[me, 2 + v:3 + v, :] = rsum(lacc)
    c1 = exchange(0, ar1)
    for cp in c1:
        cp.wait_recv()
    tot = total(ar1)
    m1 = maskf[0:1]
    lse = [tot[2:3], tot[3:4]]

    def recip(r):
        return jnp.where(m1 > 0, 1.0 / jnp.where(m1 > 0, r, 1.0), 0.0)

    a = [recip(tot[0:1]), recip(tot[1:2])]

    def sweep(a, last):
        a8 = [jnp.broadcast_to(x, (8, NS)) for x in a]
        zero = jnp.zeros((8, NS), jnp.float32)

        def body(i, carry):
            carry = list(carry)
            off = pl.multiple_of(i * CH, CH)
            for g in range(GRP):
                rows = pl.ds(off + g * 8, 8)
                for v in range(2):
                    e = e_ref[v, rows, :]
                    b = 1.0 / jnp.sum(e * a8[v], axis=1, keepdims=True)
                    eb = e * b
                    carry[v] = carry[v] + eb
                    if last:
                        bcol[v, rows, :] = jnp.broadcast_to(b, (8, 128))
                        carry[2 + v] = carry[2 + v] + eb * s_ref[1 - v, rows, :]
            return tuple(carry)
        return lax.fori_loop(0, nch, body, (zero,) * (4 if last else 2))

    r = sweep(a, False)
    for v in range(2):
        ar2[me, v:v + 1, :] = rsum(r[v])
    c2 = exchange(1, ar2)
    for cp in c2:
        cp.wait_recv()
    tot = total(ar2)
    a = [recip(tot[0:1]), recip(tot[1:2])]

    r = sweep(a, True)
    for v in range(4):
        ar3[me, v:v + 1, :] = rsum(r[v])
    c3 = exchange(2, ar3)
    eye = (lax.broadcasted_iota(jnp.int32, (128, 128), 0)
           == lax.broadcasted_iota(jnp.int32, (128, 128), 1))
    for v in range(2):
        for t in range(KLOC // 128):
            blk = bcol[v, t * 128:(t + 1) * 128, :]
            b_all[me, v:v + 1, t * 128:(t + 1) * 128] = jnp.sum(
                jnp.where(eye, blk, 0.0), axis=0, keepdims=True)
    b_copies = []
    for o, peer in enumerate(peers):
        cp = pltpu.make_async_remote_copy(
            src_ref=b_all.at[me], dst_ref=b_all.at[me], send_sem=b_send.at[o],
            recv_sem=b_recv.at[o], device_id=(peer,), device_id_type=MESH)
        cp.start()
        b_copies.append(cp)
    for cp in c3:
        cp.wait_recv()
    tot = total(ar3)
    rr = [tot[0:1], tot[1:2]]
    a = [recip(x) for x in rr]
    cnt = count[0:1]
    g = 1.0 / (2.0 * SOFT_TEMP * cnt)
    alpha = [m1 * g / x for x in lse]
    inner = sum(a[v] * (tot[2 + v:3 + v] * (1.0 / SOFT_TEMP)) - a[v] * rr[v] * jnp.log(lse[1 - v])
                for v in range(2))
    loss = -jnp.sum(jnp.where(m1 > 0, inner, 0.0), axis=1, keepdims=True) / (2.0 * cnt)
    vecs = alpha + [a[0] * g, a[1] * g]
    for i, x in enumerate(vecs):
        vecs_ref[i:i + 1, :] = x
    stat_ref[0:1, :] = jnp.broadcast_to(loss, (1, 128))
    stat_ref[1:2, :] = jnp.broadcast_to(g, (1, 128))
    meta_ref[...] = jnp.broadcast_to(cnt.astype(jnp.int32), (1, 128))

    md = m_all[me][0:1]
    cnt_before = jnp.zeros((1, 1), jnp.float32)
    for d in range(NDEV):
        cnt_before = cnt_before + jnp.where(d < me, 1.0, 0.0) * jnp.sum(m_all[d][0:1], axis=1, keepdims=True)
    pre = dot_nn(m_all[me].astype(jnp.bfloat16), tri)[0:1] + cnt_before
    pre = jnp.where(md > 0, pre, -1.0)
    pcol = jnp.sum(jnp.where(eye, jnp.broadcast_to(pre, (128, 128)), 0.0), axis=1, keepdims=True)
    lane = lax.broadcasted_iota(jnp.int32, (128, NS), 1).astype(jnp.float32)
    hit = lane == pcol
    for i, x in enumerate([a[0], a[1], alpha[0], alpha[1]]):
        col = jnp.sum(jnp.where(hit, jnp.broadcast_to(x, (128, NS)), 0.0), axis=1, keepdims=True)
        own_ref[i] = jnp.broadcast_to(col, (128, 128))

    for cp in b_copies:
        cp.wait_recv()
    b_out[...] = b_all[...]
    for cp in m_copies + z_copies[0] + z_copies[1] + fwd + c1 + c2 + c3 + b_copies:
        cp.wait_send()


def sink_call(z1, z2, m, c):
    f32, bf16 = jnp.float32, jnp.bfloat16
    vm = pl.BlockSpec(memory_space=pltpu.VMEM)
    dma = pltpu.SemaphoreType.DMA
    return pl.pallas_call(
        sink_kernel,
        in_specs=[vm, vm, vm, pl.BlockSpec(memory_space=pl.ANY)],
        out_specs=[vm] * 7,
        out_shape=[
            jax.ShapeDtypeStruct((NS, DIM), bf16),
            jax.ShapeDtypeStruct((NS, DIM), bf16),
            jax.ShapeDtypeStruct((4, NS), f32),
            jax.ShapeDtypeStruct((4, ROWS, 128), f32),
            jax.ShapeDtypeStruct((NDEV, 2, KLOC), f32),
            jax.ShapeDtypeStruct((1, 128), jnp.int32),
            jax.ShapeDtypeStruct((2, 128), f32),
        ],
        scratch_shapes=[
            pltpu.VMEM((2, NDEV, ROWS, DIM), bf16),
            pltpu.VMEM((NDEV, 8, ROWS), f32),
            pltpu.VMEM((KLOC, DIM), bf16),
            pltpu.VMEM((NS, NS), bf16),
            pltpu.VMEM((2, KLOC, NS), f32),
            pltpu.VMEM((2, KLOC, NS), f32),
            pltpu.VMEM((2, KLOC, 128), f32),
            pltpu.VMEM((NDEV, 4, NS), f32),
            pltpu.VMEM((NDEV, 2, NS), f32),
            pltpu.VMEM((NDEV, 4, NS), f32),
            pltpu.VMEM((NDEV, 2, KLOC), f32),
            dma(()), dma(()),
            dma((7,)), dma((7,)),
            dma((2, 4)), dma((2, 4)),
            dma((2, 3)), dma((2, 3)),
            dma((3, 7)), dma((3, 7)),
            dma((7,)), dma((7,)),
        ],
        compiler_params=pltpu.CompilerParams(
            collective_id=0, has_side_effects=True, vmem_limit_bytes=60 * 1024 * 1024),
        name="sinkhorn",
    )(z1, z2, m, c)


def grad_kernel(meta_ref, c_ref, zc1_ref, zc2_ref, vecs_ref, own_ref, b_ref, z1_ref, z2_ref, stat_ref,
                q1_ref, q2_ref, dz1_ref, dz2_ref, dc_ref, loss_ref,
                zz, bcol):
    step = pl.program_id(0)

    @pl.when(step == 0)
    def _():
        zz[0:ROWS] = z1_ref[...]
        zz[ROWS:2 * ROWS] = z2_ref[...]
        dz1_ref[...] = jnp.zeros_like(dz1_ref)
        dz2_ref[...] = jnp.zeros_like(dz2_ref)
        loss_ref[...] = stat_ref[0:1, :]

    g = stat_ref[1:2, 0:1]
    OS = 256
    dz = jnp.zeros((2 * ROWS, DIM), jnp.float32)
    for t in range(TK // OS):
        cols = slice(t * OS, (t + 1) * OS)
        csub = c_ref[cols, :]
        s = dot_nt(zz[...], csub)
        p = jnp.exp2(s * C_EXP)
        ps = [p[:ROWS], p[ROWS:]]
        qs = []
        for v, q_ref in enumerate((q1_ref, q2_ref)):
            arow = jnp.concatenate([own_ref[v]] * (OS // 128), axis=1)
            q = (ps[v] * ps[v] * arow) * b_ref[0, v:v + 1, cols]
            q_ref[:, cols] = q
            qs.append(q)
        gs = []
        for v in range(2):
            al = jnp.concatenate([own_ref[2 + v]] * (OS // 128), axis=1)
            gs.append((ps[v] * al - qs[1 - v] * g).astype(jnp.bfloat16))
        dz = dz + dot_nn(jnp.concatenate(gs, axis=0), csub)
    dz1_ref[...] += dz[:ROWS]
    dz2_ref[...] += dz[ROWS:]

    eye = (lax.broadcasted_iota(jnp.int32, (128, 128), 0)
           == lax.broadcasted_iota(jnp.int32, (128, 128), 1))
    for v in range(2):
        for t in range(TK // 128):
            cols = slice(t * 128, (t + 1) * 128)
            blk = jnp.where(eye, jnp.broadcast_to(b_ref[0, v:v + 1, cols], (128, 128)), 0.0)
            bcol[v, cols, :] = jnp.broadcast_to(jnp.sum(blk, axis=1, keepdims=True), (128, 128))

    dc_ref[...] = jnp.zeros_like(dc_ref)
    tiles = (meta_ref[0, 0] + (NT - 1)) // NT

    def body(i, carry):
        off = pl.multiple_of(i * NT, NT)
        z1 = zc1_ref[pl.ds(off, NT), :]
        z2 = zc2_ref[pl.ds(off, NT), :]
        vec = [vecs_ref[j:j + 1, pl.ds(off, NT)] for j in range(4)]
        for t in range(TK // SUB):
            rows = slice(t * SUB, (t + 1) * SUB)
            csub = c_ref[rows, :]
            p1 = jnp.exp2(dot_nt(csub, z1) * C_EXP)
            p2 = jnp.exp2(dot_nt(csub, z2) * C_EXP)
            b1 = jnp.concatenate([bcol[0, rows, :]] * (NT // 128), axis=1)
            b2 = jnp.concatenate([bcol[1, rows, :]] * (NT // 128), axis=1)
            g1 = (p1 * vec[0] - (p2 * p2 * b2) * vec[3]).astype(jnp.bfloat16)
            g2 = (p2 * vec[1] - (p1 * p1 * b1) * vec[2]).astype(jnp.bfloat16)
            dc_ref[rows, :] += dot_nn(g1, z1) + dot_nn(g2, z2)
        return carry
    lax.fori_loop(0, tiles, body, 0)


def grad_call(meta, c, zc1, zc2, vecs, own, b, z1, z2, stat):
    f32, bf16 = jnp.float32, jnp.bfloat16
    whole = lambda shape: pl.BlockSpec(shape, lambda i: (0,) * len(shape))
    per = KLOC // TK
    return pl.pallas_call(
        grad_kernel,
        grid=(KALL // TK,),
        in_specs=[
            pl.BlockSpec(memory_space=pltpu.SMEM),
            pl.BlockSpec((TK, DIM), lambda i: (i, 0)),
            whole((NS, DIM)), whole((NS, DIM)), whole((4, NS)), whole((4, ROWS, 128)),
            pl.BlockSpec((1, 2, TK), lambda i: (i // per, 0, i % per)),
            whole((ROWS, DIM)), whole((ROWS, DIM)), whole((2, 128)),
        ],
        out_specs=[
            pl.BlockSpec((ROWS, TK), lambda i: (0, i)),
            pl.BlockSpec((ROWS, TK), lambda i: (0, i)),
            whole((ROWS, DIM)), whole((ROWS, DIM)),
            pl.BlockSpec((TK, DIM), lambda i: (i, 0)),
            whole((1, 128)),
        ],
        out_shape=[
            jax.ShapeDtypeStruct((ROWS, KALL), f32),
            jax.ShapeDtypeStruct((ROWS, KALL), f32),
            jax.ShapeDtypeStruct((ROWS, DIM), f32),
            jax.ShapeDtypeStruct((ROWS, DIM), f32),
            jax.ShapeDtypeStruct((KALL, DIM), f32),
            jax.ShapeDtypeStruct((1, 128), f32),
        ],
        scratch_shapes=[
            pltpu.VMEM((2 * ROWS, DIM), bf16),
            pltpu.VMEM((2, TK, 128), f32),
        ],
        compiler_params=pltpu.CompilerParams(vmem_limit_bytes=60 * 1024 * 1024),
        name="grads",
    )(meta, c, zc1, zc2, vecs, own, b, z1, z2, stat)


def solution(mesh):
    def local_step(view_one, view_two, protos, valid_mask):
        zc1, zc2, vecs, own, b, meta, stat = sink_call(
            view_one, view_two, valid_mask.reshape(1, ROWS), protos)
        q1, q2, dz1, dz2, dc, loss = grad_call(
            meta, protos, zc1, zc2, vecs, own, b, view_one, view_two, stat)
        return q1, q2, loss[0, 0], dz1, dz2, dc

    return jax.shard_map(
        local_step,
        mesh=mesh,
        in_specs=(P("data", None), P("data", None), P(None, None), P("data")),
        out_specs=(P("data", None), P("data", None), P(), P("data", None), P("data", None), P(None, None)),
        check_vma=False,
    )
```

```python
import functools

import jax
import jax.numpy as jnp
from jax import lax
from jax.experimental import pallas as pl
from jax.experimental.pallas import tpu as pltpu
from jax.sharding import PartitionSpec as P

SOFT_TEMP = 0.1
LOG2E = 1.4426950408889634
C_EXP = LOG2E / SOFT_TEMP
MESH = pl.DeviceIdType.MESH
NDEV = 8
ROWS = 128
NS = NDEV * ROWS
DIM = 256
KALL = 16384
KLOC = KALL // NDEV
GRP = 128
CH = 256
TK = 2048
SUB = 512
OS = 256

NT_DIMS = (((1,), (1,)), ((), ()))


def dot_nt(x, y):
    return lax.dot_general(x, y, NT_DIMS, preferred_element_type=jnp.float32)


def dot_nn(x, y):
    return jnp.dot(x, y, preferred_element_type=jnp.float32)


def sink_kernel(z1_ref, z2_ref, m_ref, c_hbm,
                w_ref, vecs_ref, own_ref, b_out, meta_ref, stat_ref,
                z_all, m_all, cs, ps, zcs, s_ref, e_ref, bcol,
                ar1, ar1b, ar2, ar2b, ar3, ar3b, b_all,
                c_sem, loc_sem, m_send, m_recv, z_send, z_recv, f_send, f_recv,
                ar_send, ar_recv, b_send, b_recv):
    me = lax.axis_index("data")
    chip, core = me // 2, me % 2
    partner = 2 * chip + (1 - core)
    peers = [lax.rem(me + o, NDEV) for o in range(1, NDEV)]
    same = [2 * lax.rem(chip + d, 4) + core for d in range(1, 4)]

    cslice = pltpu.make_async_copy(c_hbm.at[pl.ds(me * KLOC, KLOC), :], cs, c_sem)
    cslice.start()
    m_all[me] = jnp.broadcast_to(m_ref[...].astype(jnp.float32), (8, ROWS))
    z_all[0, me] = z1_ref[...]
    z_all[1, me] = z2_ref[...]

    barrier = pltpu.get_barrier_semaphore()
    for peer in peers:
        pl.semaphore_signal(barrier, inc=1, device_id=(peer,), device_id_type=MESH)
    pl.semaphore_wait(barrier, NDEV - 1)

    m_copies = []
    for o, peer in enumerate(peers):
        cp = pltpu.make_async_remote_copy(
            src_ref=m_all.at[me], dst_ref=m_all.at[me], send_sem=m_send.at[o],
            recv_sem=m_recv.at[o], device_id=(peer,), device_id_type=MESH)
        cp.start()
        m_copies.append(cp)
    z_copies = []
    for v, src in enumerate((z1_ref, z2_ref)):
        row = []
        for d, peer in enumerate(same + [partner]):
            cp = pltpu.make_async_remote_copy(
                src_ref=src, dst_ref=z_all.at[v, me], send_sem=z_send.at[v, d],
                recv_sem=z_recv.at[v, d], device_id=(peer,), device_id_type=MESH)
            cp.start()
            row.append(cp)
        z_copies.append(row)

    for cp in m_copies:
        cp.wait_recv()

    tri = (lax.broadcasted_iota(jnp.int32, (ROWS, ROWS), 0)
           < lax.broadcasted_iota(jnp.int32, (ROWS, ROWS), 1)).astype(jnp.bfloat16)
    base = jnp.zeros((8, 1), jnp.float32)
    pos_list = []
    for d in range(NDEV):
        md = m_all[d]
        pre = dot_nn(md.astype(jnp.bfloat16), tri) + base
        pos_list.append(jnp.where(md > 0, pre, -1.0))
        base = base + jnp.sum(md, axis=1, keepdims=True)
    pos = jnp.concatenate(pos_list, axis=1)
    count = base
    mask = (lax.broadcasted_iota(jnp.int32, (8, NS), 1).astype(jnp.float32) < count)
    maskf = mask.astype(jnp.float32)
    for t in range(NS // 128):
        idx = (lax.broadcasted_iota(jnp.int32, (128, NS), 0) + t * 128).astype(jnp.float32)
        ps[t * 128:(t + 1) * 128, :] = (jnp.broadcast_to(pos[0:1], (128, NS)) == idx).astype(jnp.bfloat16)

    def forward(v):
        out = []
        for d in range(3):
            z_copies[v][d].wait_recv()
            frm = 2 * lax.rem(chip + 3 - d, 4) + core
            cp = pltpu.make_async_remote_copy(
                src_ref=z_all.at[v, frm], dst_ref=z_all.at[v, frm], send_sem=f_send.at[v, d],
                recv_sem=f_recv.at[v, d], device_id=(partner,), device_id_type=MESH)
            cp.start()
            out.append(cp)
        return out

    def compact(v, fw):
        z_copies[v][3].wait_recv()
        for cp in fw:
            cp.wait_recv()
        zv = z_all[v].reshape(NS, DIM)
        for t in range(NS // 256):
            rows = slice(t * 256, (t + 1) * 256)
            zc = dot_nn(ps[rows, :], zv).astype(jnp.bfloat16)
            zcs[v, rows, :] = zc
            w_ref[2 * t, v * ROWS:(v + 1) * ROWS, :] = zc[:ROWS]
            w_ref[2 * t + 1, v * ROWS:(v + 1) * ROWS, :] = zc[ROWS:]

    def exchange(idx, buf):
        copies = []
        for o, peer in enumerate(peers):
            cp = pltpu.make_async_remote_copy(
                src_ref=buf.at[me], dst_ref=buf.at[me], send_sem=ar_send.at[idx, o],
                recv_sem=ar_recv.at[idx, o], device_id=(peer,), device_id_type=MESH)
            cp.start()
            copies.append(cp)
        return copies

    def total(buf, copies):
        for cp in copies:
            cp.wait_recv()
        acc = buf[0]
        for d in range(1, NDEV):
            acc = acc + buf[d]
        return acc

    def rsum(x):
        return jnp.sum(x, axis=0, keepdims=True)

    m1 = maskf[0:1]

    def recip(r):
        return jnp.where(m1 > 0, 1.0 / jnp.where(m1 > 0, r, 1.0), 0.0)

    zero = jnp.zeros((8, NS), jnp.float32)

    def first_pass(v, lo, hi, carry):
        racc, lacc = carry
        for i in range(lo, hi):
            off = i * CH
            s_ref[v, off:off + CH, :] = dot_nt(cs[off:off + CH, :], zcs[v])
            for g in range(CH // 8):
                rows = slice(off + g * 8, off + g * 8 + 8)
                p = jnp.exp2(s_ref[v, rows, :] * C_EXP)
                lacc = lacc + p
                e = p * p * maskf
                e_ref[v, rows, :] = e
                b = 1.0 / jnp.sum(e, axis=1, keepdims=True)
                racc = racc + e * b
        return racc, lacc

    def sweep(v, a, last):
        a8 = jnp.broadcast_to(a, (8, NS))

        def body(i, carry):
            carry = list(carry)
            off = pl.multiple_of(i * (GRP * 8), GRP * 8)
            for g in range(GRP):
                rows = pl.ds(off + g * 8, 8)
                e = e_ref[v, rows, :]
                b = 1.0 / jnp.sum(e * a8, axis=1, keepdims=True)
                eb = e * b
                carry[0] = carry[0] + eb
                if last:
                    bcol[v, rows, :] = jnp.broadcast_to(b, (8, 128))
                    carry[1] = carry[1] + eb * s_ref[1 - v, rows, :]
            return tuple(carry)
        return lax.fori_loop(0, KLOC // (GRP * 8), body, (zero,) * (2 if last else 1))

    half = KLOC // CH // 2
    fw1 = forward(0)
    cslice.wait()
    compact(0, fw1)
    acc = first_pass(0, 0, half, (zero, zero))
    fw2 = forward(1)
    racc, lacc = first_pass(0, half, 2 * half, acc)
    ar1[me, 0:1, :] = rsum(racc)
    ar1[me, 1:2, :] = rsum(lacc)
    x1 = [exchange(0, ar1)]
    compact(1, fw2)
    racc, lacc = first_pass(1, 0, 2 * half, (zero, zero))
    ar1b[me, 0:1, :] = rsum(racc)
    ar1b[me, 1:2, :] = rsum(lacc)
    x1.append(exchange(1, ar1b))

    lse, x2 = [], []
    for v, (b1, b2) in enumerate(((ar1, ar2), (ar1b, ar2b))):
        tot = total(b1, x1[v])
        lse.append(tot[1:2])
        r, = sweep(v, recip(tot[0:1]), False)
        b2[me] = rsum(r)
        x2.append(exchange(2 + v, b2))

    x3, b_copies = [], []
    eye = (lax.broadcasted_iota(jnp.int32, (128, 128), 0)
           == lax.broadcasted_iota(jnp.int32, (128, 128), 1))
    for v, (b2, b3) in enumerate(((ar2, ar3), (ar2b, ar3b))):
        tot = total(b2, x2[v])
        r, tl = sweep(v, recip(tot), True)
        b3[me, 0:1, :] = rsum(r)
        b3[me, 1:2, :] = rsum(tl)
        x3.append(exchange(4 + v, b3))
        for t in range(KLOC // 128):
            blk = bcol[v, t * 128:(t + 1) * 128, :]
            b_all[me, v:v + 1, t * 128:(t + 1) * 128] = jnp.sum(
                jnp.where(eye, blk, 0.0), axis=0, keepdims=True)
    for o, peer in enumerate(peers):
        cp = pltpu.make_async_remote_copy(
            src_ref=b_all.at[me], dst_ref=b_all.at[me], send_sem=b_send.at[o],
            recv_sem=b_recv.at[o], device_id=(peer,), device_id_type=MESH)
        cp.start()
        b_copies.append(cp)

    cnt = count[0:1]
    g = 1.0 / (2.0 * SOFT_TEMP * cnt)
    alpha = [m1 * g / x for x in lse]
    stat_ref[1:2, :] = jnp.broadcast_to(g, (1, 128))
    meta_ref[...] = jnp.broadcast_to(cnt.astype(jnp.int32), (1, 128))
    before = jnp.zeros((1, 1), jnp.float32)
    for d in range(NDEV):
        before = before + jnp.where(d < me, 1.0, 0.0) * jnp.sum(m_all[d][0:1], axis=1, keepdims=True)
    pre = dot_nn(m_all[me].astype(jnp.bfloat16), tri)[0:1] + before
    pre = jnp.where(m_all[me][0:1] > 0, pre, -1.0)
    pcol = jnp.sum(jnp.where(eye, jnp.broadcast_to(pre, (128, 128)), 0.0), axis=1, keepdims=True)
    lane = lax.broadcasted_iota(jnp.int32, (128, NS), 1).astype(jnp.float32)
    hit = lane == pcol

    def put(i, x, scale):
        col = jnp.sum(jnp.where(hit, jnp.broadcast_to(x, (128, NS)), 0.0), axis=1, keepdims=True)
        own_ref[i] = jnp.broadcast_to(col, (128, 128))
        y = x * scale
        for t in range(NDEV):
            j = (i + 2) % 4
            vecs_ref[t, j:j + 1, :] = y[:, t * 128:(t + 1) * 128]

    put(2, alpha[0], 1.0)
    put(3, alpha[1], 1.0)

    tots = [total(ar3, x3[0])]
    a0 = recip(tots[0][0:1])
    put(0, a0, g)
    tots.append(total(ar3b, x3[1]))
    a1 = recip(tots[1][0:1])
    put(1, a1, g)
    inner = sum(a * (tots[v][1:2] * (1.0 / SOFT_TEMP)) - a * tots[v][0:1] * jnp.log(lse[1 - v])
                for v, a in enumerate((a0, a1)))
    loss = -jnp.sum(jnp.where(m1 > 0, inner, 0.0), axis=1, keepdims=True) / (2.0 * cnt)
    stat_ref[0:1, :] = jnp.broadcast_to(loss, (1, 128))

    for cp in b_copies:
        cp.wait_recv()
    b_out[...] = b_all[...]
    for cp in m_copies + z_copies[0] + z_copies[1] + fw1 + fw2 + sum(x1 + x2 + x3, []) + b_copies:
        cp.wait_send()


def sink_call(z1, z2, m, c):
    f32, bf16 = jnp.float32, jnp.bfloat16
    vm = pl.BlockSpec(memory_space=pltpu.VMEM)
    dma = pltpu.SemaphoreType.DMA
    return pl.pallas_call(
        sink_kernel,
        in_specs=[vm, vm, vm, pl.BlockSpec(memory_space=pl.ANY)],
        out_specs=[vm] * 6,
        out_shape=[
            jax.ShapeDtypeStruct((NDEV, 2 * ROWS, DIM), bf16),
            jax.ShapeDtypeStruct((NDEV, 4, ROWS), f32),
            jax.ShapeDtypeStruct((4, ROWS, 128), f32),
            jax.ShapeDtypeStruct((NDEV, 2, KLOC), f32),
            jax.ShapeDtypeStruct((1, 128), jnp.int32),
            jax.ShapeDtypeStruct((2, 128), f32),
        ],
        scratch_shapes=[
            pltpu.VMEM((2, NDEV, ROWS, DIM), bf16),
            pltpu.VMEM((NDEV, 8, ROWS), f32),
            pltpu.VMEM((KLOC, DIM), bf16),
            pltpu.VMEM((NS, NS), bf16),
            pltpu.VMEM((2, NS, DIM), bf16),
            pltpu.VMEM((2, KLOC, NS), f32),
            pltpu.VMEM((2, KLOC, NS), f32),
            pltpu.VMEM((2, KLOC, 128), f32),
            pltpu.VMEM((NDEV, 2, NS), f32),
            pltpu.VMEM((NDEV, 2, NS), f32),
            pltpu.VMEM((NDEV, 1, NS), f32),
            pltpu.VMEM((NDEV, 1, NS), f32),
            pltpu.VMEM((NDEV, 2, NS), f32),
            pltpu.VMEM((NDEV, 2, NS), f32),
            pltpu.VMEM((NDEV, 2, KLOC), f32),
            dma(()), dma(()),
            dma((7,)), dma((7,)),
            dma((2, 4)), dma((2, 4)),
            dma((2, 3)), dma((2, 3)),
            dma((6, 7)), dma((6, 7)),
            dma((7,)), dma((7,)),
        ],
        compiler_params=pltpu.CompilerParams(
            collective_id=0, has_side_effects=True, vmem_limit_bytes=60 * 1024 * 1024),
        name="sinkhorn",
    )(z1, z2, m, c)


def grad_kernel(meta_ref, c_ref, w_ref, vecs_ref, own_ref, b_ref, z1_ref, z2_ref, stat_ref,
                q1_ref, q2_ref, dz1_ref, dz2_ref, dc_ref, loss_ref,
                zz, bcol):
    step = pl.program_id(0)

    @pl.when(step == 0)
    def _():
        zz[0:ROWS] = z1_ref[...]
        zz[ROWS:2 * ROWS] = z2_ref[...]
        dz1_ref[...] = jnp.zeros_like(dz1_ref)
        dz2_ref[...] = jnp.zeros_like(dz2_ref)
        loss_ref[...] = stat_ref[0:1, :]

    g = stat_ref[1:2, 0:1]
    dz = jnp.zeros((2 * ROWS, DIM), jnp.float32)
    for t in range(TK // OS):
        cols = slice(t * OS, (t + 1) * OS)
        csub = c_ref[cols, :]
        s = dot_nt(zz[...], csub)
        p = jnp.exp2(s * C_EXP)
        ps = [p[:ROWS], p[ROWS:]]
        qs = []
        for v, q_ref in enumerate((q1_ref, q2_ref)):
            arow = jnp.concatenate([own_ref[v]] * (OS // 128), axis=1)
            q = (ps[v] * ps[v] * arow) * b_ref[0, v:v + 1, cols]
            q_ref[:, cols] = q
            qs.append(q)
        gs = []
        for v in range(2):
            al = jnp.concatenate([own_ref[2 + v]] * (OS // 128), axis=1)
            gs.append((ps[v] * al - qs[1 - v] * g).astype(jnp.bfloat16))
        dz = dz + dot_nn(jnp.concatenate(gs, axis=0), csub)
    dz1_ref[...] += dz[:ROWS]
    dz2_ref[...] += dz[ROWS:]

    eye = (lax.broadcasted_iota(jnp.int32, (128, 128), 0)
           == lax.broadcasted_iota(jnp.int32, (128, 128), 1))
    for v in range(2):
        for t in range(TK // 128):
            cols = slice(t * 128, (t + 1) * 128)
            blk = jnp.where(eye, jnp.broadcast_to(b_ref[0, v:v + 1, cols], (128, 128)), 0.0)
            bcol[v, cols, :] = jnp.broadcast_to(jnp.sum(blk, axis=1, keepdims=True), (128, 128))

    tiles = (meta_ref[0, 0] + (ROWS - 1)) // ROWS

    def piece(rows, idx):
        w = w_ref[idx]
        vec = vecs_ref[idx]
        p = jnp.exp2(dot_nt(c_ref[rows, :], w) * C_EXP)
        p1, p2 = p[:, :ROWS], p[:, ROWS:]
        g1 = p1 * vec[0:1] - (p2 * p2 * bcol[1, rows, :]) * vec[3:4]
        g2 = p2 * vec[1:2] - (p1 * p1 * bcol[0, rows, :]) * vec[2:3]
        gg = jnp.concatenate([g1.astype(jnp.bfloat16), g2.astype(jnp.bfloat16)], axis=1)
        return dot_nn(gg, w)

    pieces = [slice(t * SUB, (t + 1) * SUB) for t in range(TK // SUB)]
    for rows in pieces:
        dc_ref[rows, :] = piece(rows, 0) + piece(rows, 1)

    def body(i, carry):
        for rows in pieces:
            dc_ref[rows, :] += piece(rows, 2 * i + 2) + piece(rows, 2 * i + 3)
        return carry
    lax.fori_loop(0, (tiles - 2) // 2, body, 0)

    @pl.when(tiles % 2 == 1)
    def _():
        for rows in pieces:
            dc_ref[rows, :] += piece(rows, tiles - 1)


def grad_call(meta, c, w, vecs, own, b, z1, z2, stat):
    f32, bf16 = jnp.float32, jnp.bfloat16
    whole = lambda shape: pl.BlockSpec(shape, lambda i: (0,) * len(shape))
    per = KLOC // TK
    return pl.pallas_call(
        grad_kernel,
        grid=(KALL // TK,),
        in_specs=[
            pl.BlockSpec(memory_space=pltpu.SMEM),
            pl.BlockSpec((TK, DIM), lambda i: (i, 0)),
            whole((NDEV, 2 * ROWS, DIM)), whole((NDEV, 4, ROWS)), whole((4, ROWS, 128)),
            pl.BlockSpec((1, 2, TK), lambda i: (i // per, 0, i % per)),
            whole((ROWS, DIM)), whole((ROWS, DIM)), whole((2, 128)),
        ],
        out_specs=[
            pl.BlockSpec((ROWS, TK), lambda i: (0, i)),
            pl.BlockSpec((ROWS, TK), lambda i: (0, i)),
            whole((ROWS, DIM)), whole((ROWS, DIM)),
            pl.BlockSpec((TK, DIM), lambda i: (i, 0)),
            whole((1, 128)),
        ],
        out_shape=[
            jax.ShapeDtypeStruct((ROWS, KALL), f32),
            jax.ShapeDtypeStruct((ROWS, KALL), f32),
            jax.ShapeDtypeStruct((ROWS, DIM), f32),
            jax.ShapeDtypeStruct((ROWS, DIM), f32),
            jax.ShapeDtypeStruct((KALL, DIM), f32),
            jax.ShapeDtypeStruct((1, 128), f32),
        ],
        scratch_shapes=[
            pltpu.VMEM((2 * ROWS, DIM), bf16),
            pltpu.VMEM((2, TK, 128), f32),
        ],
        compiler_params=pltpu.CompilerParams(vmem_limit_bytes=60 * 1024 * 1024),
        name="grads",
    )(meta, c, w, vecs, own, b, z1, z2, stat)


def solution(mesh):
    def local_step(view_one, view_two, protos, valid_mask):
        w, vecs, own, b, meta, stat = sink_call(
            view_one, view_two, valid_mask.reshape(1, ROWS), protos)
        q1, q2, dz1, dz2, dc, loss = grad_call(
            meta, protos, w, vecs, own, b, view_one, view_two, stat)
        return q1, q2, loss[0, 0], dz1, dz2, dc

    return jax.shard_map(
        local_step,
        mesh=mesh,
        in_specs=(P("data", None), P("data", None), P(None, None), P("data")),
        out_specs=(P("data", None), P("data", None), P(), P("data", None), P("data", None), P(None, None)),
        check_vma=False,
    )
```

```python
import functools

import jax
import jax.numpy as jnp
from jax import lax
from jax.experimental import pallas as pl
from jax.experimental.pallas import tpu as pltpu
from jax.sharding import PartitionSpec as P

SOFT_TEMP = 0.1
LOG2E = 1.4426950408889634
C_EXP = LOG2E / SOFT_TEMP
MESH = pl.DeviceIdType.MESH
NDEV = 8
ROWS = 128
NS = NDEV * ROWS
DIM = 256
KALL = 16384
KLOC = KALL // NDEV
GRP = 128
CH = 256
TK = 4096
SUB = 256
OS = 256

PCH = 1024
NPC = KALL // PCH
NBUF = 4
SPLIT = (6, 9, 12, 14)

NT_DIMS = (((1,), (1,)), ((), ()))


def dot_nt(x, y):
    return lax.dot_general(x, y, NT_DIMS, preferred_element_type=jnp.float32)


def dot_nn(x, y):
    return jnp.dot(x, y, preferred_element_type=jnp.float32)


def sink_kernel(z1_hbm, z2_hbm, m_hbm, c_hbm,
                w_ref, vecs_ref, own_ref, b_out, meta_ref, stat_ref, p_hbm,
                z_all, m_all, cs, ps, zcs, s_ref, e_ref, bcol,
                ar1, ar1b, ar2, ar2b, ar3, ar3b, b_all, zz, cbuf, pbuf,
                c_sem, in_sem, m_send, m_recv, z_send, z_recv, f_send, f_recv,
                ar_send, ar_recv, b_send, b_recv, cb_sem, pb_sem):
    me = lax.axis_index("data")
    chip, core = me // 2, me % 2
    partner = 2 * chip + (1 - core)
    peers = [lax.rem(me + o, NDEV) for o in range(1, NDEV)]
    same = [2 * lax.rem(chip + d, 4) + core for d in range(1, 4)]

    barrier = pltpu.get_barrier_semaphore()
    for peer in peers:
        pl.semaphore_signal(barrier, inc=1, device_id=(peer,), device_id_type=MESH)

    loads = [pltpu.make_async_copy(src, dst, in_sem.at[i]) for i, (src, dst) in enumerate((
        (z1_hbm, z_all.at[0, me]), (z2_hbm, z_all.at[1, me]), (m_hbm, m_all.at[me]),
        (z1_hbm, zz.at[pl.ds(0, ROWS)]), (z2_hbm, zz.at[pl.ds(ROWS, ROWS)])))]
    for cp in loads:
        cp.start()

    def c_load(j):
        return pltpu.make_async_copy(
            c_hbm.at[pl.ds(j * PCH, PCH), :], cbuf.at[j % NBUF], cb_sem.at[j % NBUF])

    def p_store(j):
        return pltpu.make_async_copy(
            pbuf.at[j % NBUF], p_hbm.at[:, pl.ds(j * PCH, PCH)], pb_sem.at[j % NBUF])

    for j in range(NBUF):
        c_load(j).start()
    cslice = pltpu.make_async_copy(c_hbm.at[pl.ds(me * KLOC, KLOC), :], cs, c_sem)
    cslice.start()

    def own_scores(lo, hi):
        for j in range(lo, hi):
            c_load(j).wait()
            if j >= NBUF:
                p_store(j - NBUF).wait()
            for t in range(PCH // 256):
                cols = slice(t * 256, (t + 1) * 256)
                sc = dot_nt(zz[...], cbuf[j % NBUF, cols, :])
                pbuf[j % NBUF, :, cols] = jnp.exp2(sc * C_EXP)
            p_store(j).start()
            if j + NBUF < NPC:
                c_load(j + NBUF).start()

    for cp in loads:
        cp.wait()
    pl.semaphore_wait(barrier, NDEV - 1)

    m_copies = []
    for o, peer in enumerate(peers):
        cp = pltpu.make_async_remote_copy(
            src_ref=m_all.at[me], dst_ref=m_all.at[me], send_sem=m_send.at[o],
            recv_sem=m_recv.at[o], device_id=(peer,), device_id_type=MESH)
        cp.start()
        m_copies.append(cp)
    z_copies = []
    for v in range(2):
        row = []
        for d, peer in enumerate(same + [partner]):
            cp = pltpu.make_async_remote_copy(
                src_ref=z_all.at[v, me], dst_ref=z_all.at[v, me], send_sem=z_send.at[v, d],
                recv_sem=z_recv.at[v, d], device_id=(peer,), device_id_type=MESH)
            cp.start()
            row.append(cp)
        z_copies.append(row)

    own_scores(0, SPLIT[0])
    for cp in m_copies:
        cp.wait_recv()
    mf = [jnp.broadcast_to(m_all[d].astype(jnp.float32), (8, ROWS)) for d in range(NDEV)]

    tri = (lax.broadcasted_iota(jnp.int32, (ROWS, ROWS), 0)
           < lax.broadcasted_iota(jnp.int32, (ROWS, ROWS), 1)).astype(jnp.bfloat16)
    base = jnp.zeros((8, 1), jnp.float32)
    pos_list = []
    for d in range(NDEV):
        md = mf[d]
        pre = dot_nn(md.astype(jnp.bfloat16), tri) + base
        pos_list.append(jnp.where(md > 0, pre, -1.0))
        base = base + jnp.sum(md, axis=1, keepdims=True)
    pos = jnp.concatenate(pos_list, axis=1)
    count = base
    mask = (lax.broadcasted_iota(jnp.int32, (8, NS), 1).astype(jnp.float32) < count)
    maskf = mask.astype(jnp.float32)
    for t in range(NS // 128):
        idx = (lax.broadcasted_iota(jnp.int32, (128, NS), 0) + t * 128).astype(jnp.float32)
        ps[t * 128:(t + 1) * 128, :] = (jnp.broadcast_to(pos[0:1], (128, NS)) == idx).astype(jnp.bfloat16)

    def forward(v):
        out = []
        for d in range(3):
            z_copies[v][d].wait_recv()
            frm = 2 * lax.rem(chip + 3 - d, 4) + core
            cp = pltpu.make_async_remote_copy(
                src_ref=z_all.at[v, frm], dst_ref=z_all.at[v, frm], send_sem=f_send.at[v, d],
                recv_sem=f_recv.at[v, d], device_id=(partner,), device_id_type=MESH)
            cp.start()
            out.append(cp)
        return out

    def compact(v, fw):
        z_copies[v][3].wait_recv()
        for cp in fw:
            cp.wait_recv()
        zv = z_all[v].reshape(NS, DIM)
        for t in range(NS // 256):
            rows = slice(t * 256, (t + 1) * 256)
            zc = dot_nn(ps[rows, :], zv).astype(jnp.bfloat16)
            zcs[v, rows, :] = zc
            w_ref[2 * t, v * ROWS:(v + 1) * ROWS, :] = zc[:ROWS]
            w_ref[2 * t + 1, v * ROWS:(v + 1) * ROWS, :] = zc[ROWS:]

    def exchange(idx, buf):
        copies = []
        for o, peer in enumerate(peers):
            cp = pltpu.make_async_remote_copy(
                src_ref=buf.at[me], dst_ref=buf.at[me], send_sem=ar_send.at[idx, o],
                recv_sem=ar_recv.at[idx, o], device_id=(peer,), device_id_type=MESH)
            cp.start()
            copies.append(cp)
        return copies

    def total(buf, copies):
        for cp in copies:
            cp.wait_recv()
        acc = buf[0]
        for d in range(1, NDEV):
            acc = acc + buf[d]
        return acc

    def rsum(x):
        return jnp.sum(x, axis=0, keepdims=True)

    m1 = maskf[0:1]

    def recip(r):
        return jnp.where(m1 > 0, 1.0 / jnp.where(m1 > 0, r, 1.0), 0.0)

    zero = jnp.zeros((8, NS), jnp.float32)

    def first_pass(v, lo, hi, carry):
        racc, lacc = carry

        def rows_part(i, racc):
            for g in range(CH // 8):
                rows = slice(i * CH + g * 8, i * CH + g * 8 + 8)
                b = jnp.concatenate([bcol[v, rows, :]] * (NS // 128), axis=1)
                racc = racc + e_ref[v, rows, :] * b
            return racc

        for i in range(lo, hi):
            off = i * CH
            s_ref[v, off:off + CH, :] = dot_nt(cs[off:off + CH, :], zcs[v])
            for g in range(CH // 8):
                rows = slice(off + g * 8, off + g * 8 + 8)
                p = jnp.exp2(s_ref[v, rows, :] * C_EXP)
                lacc = lacc + p
                e = p * p * maskf
                e_ref[v, rows, :] = e
                bcol[v, rows, :] = jnp.broadcast_to(1.0 / jnp.sum(e, axis=1, keepdims=True), (8, 128))
            if i > lo:
                racc = rows_part(i - 1, racc)
        return rows_part(hi - 1, racc), lacc

    def sweep(v, a, last):
        a8 = jnp.broadcast_to(a, (8, NS))

        def body(i, carry):
            carry = list(carry)
            off = pl.multiple_of(i * (GRP * 8), GRP * 8)
            for g in range(GRP):
                rows = pl.ds(off + g * 8, 8)
                e = e_ref[v, rows, :]
                b = 1.0 / jnp.sum(e * a8, axis=1, keepdims=True)
                eb = e * b
                carry[0] = carry[0] + eb
                if last:
                    bcol[v, rows, :] = jnp.broadcast_to(b, (8, 128))
                    carry[1] = carry[1] + eb * s_ref[1 - v, rows, :]
            return tuple(carry)
        return lax.fori_loop(0, KLOC // (GRP * 8), body, (zero,) * (2 if last else 1))

    half = KLOC // CH // 2
    fw1 = forward(0)
    own_scores(SPLIT[0], SPLIT[1])
    cslice.wait()
    compact(0, fw1)
    acc = first_pass(0, 0, half, (zero, zero))
    fw2 = forward(1)
    racc, lacc = first_pass(0, half, 2 * half, acc)
    ar1[me, 0:1, :] = rsum(racc)
    ar1[me, 1:2, :] = rsum(lacc)
    x1 = [exchange(0, ar1)]
    compact(1, fw2)
    racc, lacc = first_pass(1, 0, 2 * half, (zero, zero))
    ar1b[me, 0:1, :] = rsum(racc)
    ar1b[me, 1:2, :] = rsum(lacc)
    x1.append(exchange(1, ar1b))

    lse, x2 = [], []
    for v, (b1, b2) in enumerate(((ar1, ar2), (ar1b, ar2b))):
        if v == 1:
            own_scores(SPLIT[1], SPLIT[2])
        tot = total(b1, x1[v])
        lse.append(tot[1:2])
        r, = sweep(v, recip(tot[0:1]), False)
        b2[me] = rsum(r)
        x2.append(exchange(2 + v, b2))

    x3, b_copies = [], []
    eye = (lax.broadcasted_iota(jnp.int32, (128, 128), 0)
           == lax.broadcasted_iota(jnp.int32, (128, 128), 1))
    for v, (b2, b3) in enumerate(((ar2, ar3), (ar2b, ar3b))):
        if v == 1:
            own_scores(SPLIT[2], SPLIT[3])
        tot = total(b2, x2[v])
        r, tl = sweep(v, recip(tot), True)
        b3[me, 0:1, :] = rsum(r)
        b3[me, 1:2, :] = rsum(tl)
        x3.append(exchange(4 + v, b3))
        for t in range(KLOC // 128):
            blk = bcol[v, t * 128:(t + 1) * 128, :]
            b_all[me, v:v + 1, t * 128:(t + 1) * 128] = jnp.sum(
                jnp.where(eye, blk, 0.0), axis=0, keepdims=True)
    for o, peer in enumerate(peers):
        cp = pltpu.make_async_remote_copy(
            src_ref=b_all.at[me], dst_ref=b_all.at[me], send_sem=b_send.at[o],
            recv_sem=b_recv.at[o], device_id=(peer,), device_id_type=MESH)
        cp.start()
        b_copies.append(cp)

    cnt = count[0:1]
    g = 1.0 / (2.0 * SOFT_TEMP * cnt)
    alpha = [m1 * g / x for x in lse]
    stat_ref[1:2, :] = jnp.broadcast_to(g, (1, 128))
    meta_ref[...] = jnp.broadcast_to(cnt.astype(jnp.int32), (1, 128))
    before = jnp.zeros((1, 1), jnp.float32)
    for d in range(NDEV):
        before = before + jnp.where(d < me, 1.0, 0.0) * jnp.sum(mf[d][0:1], axis=1, keepdims=True)
    mine = jnp.broadcast_to(m_all[me].astype(jnp.float32), (8, ROWS))
    pre = dot_nn(mine.astype(jnp.bfloat16), tri)[0:1] + before
    pre = jnp.where(mine[0:1] > 0, pre, -1.0)
    pcol = jnp.sum(jnp.where(eye, jnp.broadcast_to(pre, (128, 128)), 0.0), axis=1, keepdims=True)
    lane = lax.broadcasted_iota(jnp.int32, (128, NS), 1).astype(jnp.float32)
    hit = lane == pcol

    def put(i, x, scale):
        col = jnp.sum(jnp.where(hit, jnp.broadcast_to(x, (128, NS)), 0.0), axis=1, keepdims=True)
        own_ref[i] = jnp.broadcast_to(col, (128, 128))
        y = x * scale
        for t in range(NDEV):
            j = (i + 2) % 4
            vecs_ref[t, j:j + 1, :] = y[:, t * 128:(t + 1) * 128]

    put(2, alpha[0], 1.0)
    put(3, alpha[1], 1.0)
    own_scores(SPLIT[3], NPC)

    tots = [total(ar3, x3[0])]
    a0 = recip(tots[0][0:1])
    put(0, a0, g)
    tots.append(total(ar3b, x3[1]))
    a1 = recip(tots[1][0:1])
    put(1, a1, g)
    inner = sum(a * (tots[v][1:2] * (1.0 / SOFT_TEMP)) - a * tots[v][0:1] * jnp.log(lse[1 - v])
                for v, a in enumerate((a0, a1)))
    loss = -jnp.sum(jnp.where(m1 > 0, inner, 0.0), axis=1, keepdims=True) / (2.0 * cnt)
    stat_ref[0:1, :] = jnp.broadcast_to(loss, (1, 128))

    for cp in b_copies:
        cp.wait_recv()
    for d in range(NDEV):
        b_out[:, d * KLOC:(d + 1) * KLOC] = b_all[d]
    for j in range(NPC - NBUF, NPC):
        p_store(j).wait()
    for cp in m_copies + z_copies[0] + z_copies[1] + fw1 + fw2 + sum(x1 + x2 + x3, []) + b_copies:
        cp.wait_send()


def sink_call(z1, z2, m, c):
    f32, bf16 = jnp.float32, jnp.bfloat16
    vm = pl.BlockSpec(memory_space=pltpu.VMEM)
    hbm = pl.BlockSpec(memory_space=pl.ANY)
    dma = pltpu.SemaphoreType.DMA
    return pl.pallas_call(
        sink_kernel,
        in_specs=[hbm] * 4,
        out_specs=[vm] * 6 + [hbm],
        out_shape=[
            jax.ShapeDtypeStruct((NDEV, 2 * ROWS, DIM), bf16),
            jax.ShapeDtypeStruct((NDEV, 4, ROWS), f32),
            jax.ShapeDtypeStruct((4, ROWS, 128), f32),
            jax.ShapeDtypeStruct((2, KALL), f32),
            jax.ShapeDtypeStruct((1, 128), jnp.int32),
            jax.ShapeDtypeStruct((2, 128), f32),
            jax.ShapeDtypeStruct((2 * ROWS, KALL), f32),
        ],
        scratch_shapes=[
            pltpu.VMEM((2, NDEV, ROWS, DIM), bf16),
            pltpu.VMEM((NDEV, 1, ROWS), jnp.int32),
            pltpu.VMEM((KLOC, DIM), bf16),
            pltpu.VMEM((NS, NS), bf16),
            pltpu.VMEM((2, NS, DIM), bf16),
            pltpu.VMEM((2, KLOC, NS), f32),
            pltpu.VMEM((2, KLOC, NS), f32),
            pltpu.VMEM((2, KLOC, 128), f32),
            pltpu.VMEM((NDEV, 2, NS), f32),
            pltpu.VMEM((NDEV, 2, NS), f32),
            pltpu.VMEM((NDEV, 1, NS), f32),
            pltpu.VMEM((NDEV, 1, NS), f32),
            pltpu.VMEM((NDEV, 2, NS), f32),
            pltpu.VMEM((NDEV, 2, NS), f32),
            pltpu.VMEM((NDEV, 2, KLOC), f32),
            pltpu.VMEM((2 * ROWS, DIM), bf16),
            pltpu.VMEM((NBUF, PCH, DIM), bf16),
            pltpu.VMEM((NBUF, 2 * ROWS, PCH), f32),
            dma(()), dma((5,)),
            dma((7,)), dma((7,)),
            dma((2, 4)), dma((2, 4)),
            dma((2, 3)), dma((2, 3)),
            dma((6, 7)), dma((6, 7)),
            dma((7,)), dma((7,)),
            dma((NBUF,)), dma((NBUF,)),
        ],
        compiler_params=pltpu.CompilerParams(
            collective_id=0, has_side_effects=True, vmem_limit_bytes=60 * 1024 * 1024),
        name="sinkhorn",
    )(z1, z2, m, c)


def grad_kernel(meta_ref, c_ref, w_ref, vecs_ref, own_ref, b_ref, p_ref, stat_ref,
                q1_ref, q2_ref, dz1_ref, dz2_ref, dc_ref, loss_ref,
                bcol):
    step = pl.program_id(0)

    @pl.when(step == 0)
    def _():
        dz1_ref[...] = jnp.zeros_like(dz1_ref)
        dz2_ref[...] = jnp.zeros_like(dz2_ref)
        loss_ref[...] = stat_ref[0:1, :]

    g = stat_ref[1:2, 0:1]
    dz = jnp.zeros((2 * ROWS, DIM), jnp.float32)
    for t in range(TK // OS):
        cols = slice(t * OS, (t + 1) * OS)
        ps = [p_ref[:ROWS, cols], p_ref[ROWS:, cols]]
        qs = []
        for v, q_ref in enumerate((q1_ref, q2_ref)):
            arow = jnp.concatenate([own_ref[v]] * (OS // 128), axis=1)
            q = (ps[v] * ps[v] * arow) * b_ref[v:v + 1, cols]
            q_ref[:, cols] = q
            qs.append(q)
        gs = []
        for v in range(2):
            al = jnp.concatenate([own_ref[2 + v]] * (OS // 128), axis=1)
            gs.append((ps[v] * al - qs[1 - v] * g).astype(jnp.bfloat16))
        dz = dz + dot_nn(jnp.concatenate(gs, axis=0), c_ref[cols, :])
    dz1_ref[...] += dz[:ROWS]
    dz2_ref[...] += dz[ROWS:]

    eye = (lax.broadcasted_iota(jnp.int32, (128, 128), 0)
           == lax.broadcasted_iota(jnp.int32, (128, 128), 1))
    for v in range(2):
        for t in range(TK // 128):
            cols = slice(t * 128, (t + 1) * 128)
            blk = jnp.where(eye, jnp.broadcast_to(b_ref[v:v + 1, cols], (128, 128)), 0.0)
            bcol[v, cols, :] = jnp.broadcast_to(jnp.sum(blk, axis=1, keepdims=True), (128, 128))

    tiles = (meta_ref[0, 0] + (ROWS - 1)) // ROWS

    def piece(rows, idx):
        w = w_ref[idx]
        vec = vecs_ref[idx]
        p = jnp.exp2(dot_nt(c_ref[rows, :], w) * C_EXP)
        p1, p2 = p[:, :ROWS], p[:, ROWS:]
        g1 = p1 * vec[0:1] - (p2 * p2 * bcol[1, rows, :]) * vec[3:4]
        g2 = p2 * vec[1:2] - (p1 * p1 * bcol[0, rows, :]) * vec[2:3]
        gg = jnp.concatenate([g1.astype(jnp.bfloat16), g2.astype(jnp.bfloat16)], axis=1)
        return dot_nn(gg, w)

    pieces = [slice(t * SUB, (t + 1) * SUB) for t in range(TK // SUB)]
    for rows in pieces:
        dc_ref[rows, :] = piece(rows, 0) + piece(rows, 1)

    def body(i, carry):
        for rows in pieces:
            dc_ref[rows, :] += piece(rows, 2 * i + 2) + piece(rows, 2 * i + 3)
        return carry
    lax.fori_loop(0, (tiles - 2) // 2, body, 0)

    @pl.when(tiles % 2 == 1)
    def _():
        for rows in pieces:
            dc_ref[rows, :] += piece(rows, tiles - 1)


def grad_call(meta, c, w, vecs, own, b, p, stat):
    f32, bf16 = jnp.float32, jnp.bfloat16
    whole = lambda shape: pl.BlockSpec(shape, lambda i: (0,) * len(shape))
    return pl.pallas_call(
        grad_kernel,
        grid=(KALL // TK,),
        in_specs=[
            pl.BlockSpec(memory_space=pltpu.SMEM),
            pl.BlockSpec((TK, DIM), lambda i: (i, 0)),
            whole((NDEV, 2 * ROWS, DIM)), whole((NDEV, 4, ROWS)), whole((4, ROWS, 128)),
            pl.BlockSpec((2, TK), lambda i: (0, i)),
            pl.BlockSpec((2 * ROWS, TK), lambda i: (0, i)),
            whole((2, 128)),
        ],
        out_specs=[
            pl.BlockSpec((ROWS, TK), lambda i: (0, i)),
            pl.BlockSpec((ROWS, TK), lambda i: (0, i)),
            whole((ROWS, DIM)), whole((ROWS, DIM)),
            pl.BlockSpec((TK, DIM), lambda i: (i, 0)),
            whole((1, 128)),
        ],
        out_shape=[
            jax.ShapeDtypeStruct((ROWS, KALL), f32),
            jax.ShapeDtypeStruct((ROWS, KALL), f32),
            jax.ShapeDtypeStruct((ROWS, DIM), f32),
            jax.ShapeDtypeStruct((ROWS, DIM), f32),
            jax.ShapeDtypeStruct((KALL, DIM), f32),
            jax.ShapeDtypeStruct((1, 128), f32),
        ],
        scratch_shapes=[
            pltpu.VMEM((2, TK, 128), f32),
        ],
        compiler_params=pltpu.CompilerParams(vmem_limit_bytes=60 * 1024 * 1024),
        name="grads",
    )(meta, c, w, vecs, own, b, p, stat)


def solution(mesh):
    def local_step(view_one, view_two, protos, valid_mask):
        w, vecs, own, b, meta, stat, p = sink_call(
            view_one, view_two, valid_mask.reshape(1, ROWS), protos)
        q1, q2, dz1, dz2, dc, loss = grad_call(
            meta, protos, w, vecs, own, b, p, stat)
        return q1, q2, loss[0, 0], dz1, dz2, dc

    return jax.shard_map(
        local_step,
        mesh=mesh,
        in_specs=(P("data", None), P("data", None), P(None, None), P("data")),
        out_specs=(P("data", None), P("data", None), P(), P("data", None), P("data", None), P(None, None)),
        check_vma=False,
    )
```

```python
import functools

import jax
import jax.numpy as jnp
from jax import lax
from jax.experimental import pallas as pl
from jax.experimental.pallas import tpu as pltpu
from jax.sharding import PartitionSpec as P

SOFT_TEMP = 0.1
LOG2E = 1.4426950408889634
C_EXP = LOG2E / SOFT_TEMP
MESH = pl.DeviceIdType.MESH
NDEV = 8
ROWS = 128
NS = NDEV * ROWS
DIM = 256
KALL = 16384
KLOC = KALL // NDEV
GRP = 128
CH = 256
TK = 4096
SUB = 256
CK = 1024
OS = 256

PCH = 1024
NPC = KALL // PCH
NBUF = 4
SPLIT = (10, 12, 14, 16)

VM1 = 56
VM2 = 50
NT_DIMS = (((1,), (1,)), ((), ()))


def dot_nt(x, y):
    return lax.dot_general(x, y, NT_DIMS, preferred_element_type=jnp.float32)


def dot_nn(x, y):
    return jnp.dot(x, y, preferred_element_type=jnp.float32)


def sink_kernel(z1_hbm, z2_hbm, m_hbm, c_hbm,
                w_ref, vecs_ref, own_ref, b_out, stat_ref, p_hbm,
                z_all, m_all, cs, ps, zcs, s_ref, e_ref, bcol,
                ar1, ar1b, ar2, ar2b, ar3, ar3b, b_all, zz, cbuf, pbuf,
                c_sem, in_sem, m_send, m_recv, z_send, z_recv, f_send, f_recv,
                ar_send, ar_recv, b_send, b_recv, cb_sem, pb_sem):
    me = lax.axis_index("data")
    chip, core = me // 2, me % 2
    partner = 2 * chip + (1 - core)
    peers = [lax.rem(me + o, NDEV) for o in range(1, NDEV)]
    same = [2 * lax.rem(chip + d, 4) + core for d in range(1, 4)]

    barrier = pltpu.get_barrier_semaphore()
    for peer in peers:
        pl.semaphore_signal(barrier, inc=1, device_id=(peer,), device_id_type=MESH)

    loads = [pltpu.make_async_copy(src, dst, in_sem.at[i]) for i, (src, dst) in enumerate((
        (z1_hbm, z_all.at[0, me]), (z2_hbm, z_all.at[1, me]), (m_hbm, m_all.at[me]),
        (z1_hbm, zz.at[pl.ds(0, ROWS)]), (z2_hbm, zz.at[pl.ds(ROWS, ROWS)])))]
    for cp in loads:
        cp.start()

    def c_load(j):
        return pltpu.make_async_copy(
            c_hbm.at[pl.ds(j * PCH, PCH), :], cbuf.at[j % NBUF], cb_sem.at[j % NBUF])

    def p_store(j):
        return pltpu.make_async_copy(
            pbuf.at[j % NBUF], p_hbm.at[:, pl.ds(j * PCH, PCH)], pb_sem.at[j % NBUF])

    for j in range(NBUF):
        c_load(j).start()
    cslice = pltpu.make_async_copy(c_hbm.at[pl.ds(me * KLOC, KLOC), :], cs, c_sem)
    cslice.start()

    def own_scores(lo, hi):
        for j in range(lo, hi):
            c_load(j).wait()
            if j >= NBUF:
                p_store(j - NBUF).wait()
            for t in range(PCH // 256):
                cols = slice(t * 256, (t + 1) * 256)
                sc = dot_nt(zz[...], cbuf[j % NBUF, cols, :])
                pbuf[j % NBUF, :, cols] = jnp.exp2(sc * C_EXP)
            p_store(j).start()
            if j + NBUF < NPC:
                c_load(j + NBUF).start()

    for cp in loads:
        cp.wait()
    pl.semaphore_wait(barrier, NDEV - 1)

    m_copies = []
    for o, peer in enumerate(peers):
        cp = pltpu.make_async_remote_copy(
            src_ref=m_all.at[me], dst_ref=m_all.at[me], send_sem=m_send.at[o],
            recv_sem=m_recv.at[o], device_id=(peer,), device_id_type=MESH)
        cp.start()
        m_copies.append(cp)
    z_copies = []
    for v in range(2):
        row = []
        for d, peer in enumerate(same + [partner]):
            cp = pltpu.make_async_remote_copy(
                src_ref=z_all.at[v, me], dst_ref=z_all.at[v, me], send_sem=z_send.at[v, d],
                recv_sem=z_recv.at[v, d], device_id=(peer,), device_id_type=MESH)
            cp.start()
            row.append(cp)
        z_copies.append(row)

    own_scores(0, SPLIT[0])
    for cp in m_copies:
        cp.wait_recv()
    mf = [jnp.broadcast_to(m_all[d].astype(jnp.float32), (8, ROWS)) for d in range(NDEV)]

    tri = (lax.broadcasted_iota(jnp.int32, (ROWS, ROWS), 0)
           < lax.broadcasted_iota(jnp.int32, (ROWS, ROWS), 1)).astype(jnp.bfloat16)
    base = jnp.zeros((8, 1), jnp.float32)
    pos_list = []
    for d in range(NDEV):
        md = mf[d]
        pre = dot_nn(md.astype(jnp.bfloat16), tri) + base
        pos_list.append(jnp.where(md > 0, pre, -1.0))
        base = base + jnp.sum(md, axis=1, keepdims=True)
    pos = jnp.concatenate(pos_list, axis=1)
    count = base
    mask = (lax.broadcasted_iota(jnp.int32, (8, NS), 1).astype(jnp.float32) < count)
    maskf = mask.astype(jnp.float32)
    for t in range(NS // 128):
        idx = (lax.broadcasted_iota(jnp.int32, (128, NS), 0) + t * 128).astype(jnp.float32)
        ps[t * 128:(t + 1) * 128, :] = (jnp.broadcast_to(pos[0:1], (128, NS)) == idx).astype(jnp.bfloat16)

    def forward(v):
        out = []
        for d in range(3):
            z_copies[v][d].wait_recv()
            frm = 2 * lax.rem(chip + 3 - d, 4) + core
            cp = pltpu.make_async_remote_copy(
                src_ref=z_all.at[v, frm], dst_ref=z_all.at[v, frm], send_sem=f_send.at[v, d],
                recv_sem=f_recv.at[v, d], device_id=(partner,), device_id_type=MESH)
            cp.start()
            out.append(cp)
        return out

    def compact(v, fw):
        z_copies[v][3].wait_recv()
        for cp in fw:
            cp.wait_recv()
        zv = z_all[v].reshape(NS, DIM)
        for t in range(NS // 256):
            rows = slice(t * 256, (t + 1) * 256)
            zc = dot_nn(ps[rows, :], zv).astype(jnp.bfloat16)
            zcs[v, rows, :] = zc
            w_ref[2 * t, v * ROWS:(v + 1) * ROWS, :] = zc[:ROWS]
            w_ref[2 * t + 1, v * ROWS:(v + 1) * ROWS, :] = zc[ROWS:]

    def exchange(idx, buf):
        copies = []
        for o, peer in enumerate(peers):
            cp = pltpu.make_async_remote_copy(
                src_ref=buf.at[me], dst_ref=buf.at[me], send_sem=ar_send.at[idx, o],
                recv_sem=ar_recv.at[idx, o], device_id=(peer,), device_id_type=MESH)
            cp.start()
            copies.append(cp)
        return copies

    def total(buf, copies):
        for cp in copies:
            cp.wait_recv()
        acc = buf[0]
        for d in range(1, NDEV):
            acc = acc + buf[d]
        return acc

    def rsum(x):
        return jnp.sum(x, axis=0, keepdims=True)

    m1 = maskf[0:1]

    def recip(r):
        return jnp.where(m1 > 0, 1.0 / jnp.where(m1 > 0, r, 1.0), 0.0)

    zero = jnp.zeros((8, NS), jnp.float32)

    def first_pass(v, lo, hi, carry):
        racc, lacc = carry

        def rows_part(i, racc):
            for g in range(CH // 8):
                rows = slice(i * CH + g * 8, i * CH + g * 8 + 8)
                b = jnp.concatenate([bcol[v, rows, :]] * (NS // 128), axis=1)
                racc = racc + e_ref[v, rows, :] * b
            return racc

        for i in range(lo, hi):
            off = i * CH
            s_ref[v, off:off + CH, :] = dot_nt(cs[off:off + CH, :], zcs[v])
            for g in range(CH // 8):
                rows = slice(off + g * 8, off + g * 8 + 8)
                p = jnp.exp2(s_ref[v, rows, :] * C_EXP)
                lacc = lacc + p
                e = p * p * maskf
                e_ref[v, rows, :] = e
                bcol[v, rows, :] = jnp.broadcast_to(1.0 / jnp.sum(e, axis=1, keepdims=True), (8, 128))
            if i > lo:
                racc = rows_part(i - 1, racc)
        return rows_part(hi - 1, racc), lacc

    def sweep(v, a, last):
        a8 = jnp.broadcast_to(a, (8, NS))

        def body(i, carry):
            carry = list(carry)
            off = pl.multiple_of(i * (GRP * 8), GRP * 8)
            for g in range(GRP):
                rows = pl.ds(off + g * 8, 8)
                e = e_ref[v, rows, :]
                b = 1.0 / jnp.sum(e * a8, axis=1, keepdims=True)
                eb = e * b
                carry[0] = carry[0] + eb
                if last:
                    bcol[v, rows, :] = jnp.broadcast_to(b, (8, 128))
                    carry[1] = carry[1] + eb * s_ref[1 - v, rows, :]
            return tuple(carry)
        return lax.fori_loop(0, KLOC // (GRP * 8), body, (zero,) * (2 if last else 1))

    half = KLOC // CH // 2
    fw1 = forward(0)
    own_scores(SPLIT[0], SPLIT[1])
    cslice.wait()
    compact(0, fw1)
    acc = first_pass(0, 0, half, (zero, zero))
    fw2 = forward(1)
    racc, lacc = first_pass(0, half, 2 * half, acc)
    ar1[me, 0:1, :] = rsum(racc)
    ar1[me, 1:2, :] = rsum(lacc)
    x1 = [exchange(0, ar1)]
    compact(1, fw2)
    racc, lacc = first_pass(1, 0, 2 * half, (zero, zero))
    ar1b[me, 0:1, :] = rsum(racc)
    ar1b[me, 1:2, :] = rsum(lacc)
    x1.append(exchange(1, ar1b))

    lse, x2 = [], []
    for v, (b1, b2) in enumerate(((ar1, ar2), (ar1b, ar2b))):
        if v == 1:
            own_scores(SPLIT[1], SPLIT[2])
        tot = total(b1, x1[v])
        lse.append(tot[1:2])
        r, = sweep(v, recip(tot[0:1]), False)
        b2[me] = rsum(r)
        x2.append(exchange(2 + v, b2))

    x3, b_copies = [], []
    eye = (lax.broadcasted_iota(jnp.int32, (128, 128), 0)
           == lax.broadcasted_iota(jnp.int32, (128, 128), 1))
    for v, (b2, b3) in enumerate(((ar2, ar3), (ar2b, ar3b))):
        if v == 1:
            own_scores(SPLIT[2], SPLIT[3])
        tot = total(b2, x2[v])
        r, tl = sweep(v, recip(tot), True)
        b3[me, 0:1, :] = rsum(r)
        b3[me, 1:2, :] = rsum(tl)
        x3.append(exchange(4 + v, b3))
        for t in range(KLOC // 128):
            blk = bcol[v, t * 128:(t + 1) * 128, :]
            b_all[me, v:v + 1, t * 128:(t + 1) * 128] = jnp.sum(
                jnp.where(eye, blk, 0.0), axis=0, keepdims=True)
    for o, peer in enumerate(peers):
        cp = pltpu.make_async_remote_copy(
            src_ref=b_all.at[me], dst_ref=b_all.at[me], send_sem=b_send.at[o],
            recv_sem=b_recv.at[o], device_id=(peer,), device_id_type=MESH)
        cp.start()
        b_copies.append(cp)

    cnt = count[0:1]
    g = 1.0 / (2.0 * SOFT_TEMP * cnt)
    alpha = [m1 * g / x for x in lse]
    stat_ref[1:2, :] = jnp.broadcast_to(g, (1, 128))
    stat_ref[2:3, :] = jnp.broadcast_to(cnt, (1, 128))
    before = jnp.zeros((1, 1), jnp.float32)
    for d in range(NDEV):
        before = before + jnp.where(d < me, 1.0, 0.0) * jnp.sum(mf[d][0:1], axis=1, keepdims=True)
    mine = jnp.broadcast_to(m_all[me].astype(jnp.float32), (8, ROWS))
    pre = dot_nn(mine.astype(jnp.bfloat16), tri)[0:1] + before
    pre = jnp.where(mine[0:1] > 0, pre, -1.0)
    pcol = jnp.sum(jnp.where(eye, jnp.broadcast_to(pre, (128, 128)), 0.0), axis=1, keepdims=True)
    lane = lax.broadcasted_iota(jnp.int32, (128, NS), 1).astype(jnp.float32)
    hit = lane == pcol

    def put(i, x, scale):
        col = jnp.sum(jnp.where(hit, jnp.broadcast_to(x, (128, NS)), 0.0), axis=1, keepdims=True)
        own_ref[i] = jnp.broadcast_to(col, (128, 128))
        y = x * scale
        for t in range(NDEV):
            j = (i + 2) % 4
            vecs_ref[t, j:j + 1, :] = y[:, t * 128:(t + 1) * 128]

    put(2, alpha[0], 1.0)
    put(3, alpha[1], 1.0)
    own_scores(SPLIT[3], NPC)

    tots = [total(ar3, x3[0])]
    a0 = recip(tots[0][0:1])
    put(0, a0, g)
    tots.append(total(ar3b, x3[1]))
    a1 = recip(tots[1][0:1])
    put(1, a1, g)
    inner = sum(a * (tots[v][1:2] * (1.0 / SOFT_TEMP)) - a * tots[v][0:1] * jnp.log(lse[1 - v])
                for v, a in enumerate((a0, a1)))
    loss = -jnp.sum(jnp.where(m1 > 0, inner, 0.0), axis=1, keepdims=True) / (2.0 * cnt)
    stat_ref[0:1, :] = jnp.broadcast_to(loss, (1, 128))

    for cp in b_copies:
        cp.wait_recv()
    for d in range(NDEV):
        b_out[:, d * KLOC:(d + 1) * KLOC] = b_all[d]
    for j in range(NPC - NBUF, NPC):
        p_store(j).wait()
    for cp in m_copies + z_copies[0] + z_copies[1] + fw1 + fw2 + sum(x1 + x2 + x3, []) + b_copies:
        cp.wait_send()


def sink_call(z1, z2, m, c):
    f32, bf16 = jnp.float32, jnp.bfloat16
    vm = pl.BlockSpec(memory_space=pltpu.VMEM)
    hbm = pl.BlockSpec(memory_space=pltpu.HBM)
    dma = pltpu.SemaphoreType.DMA
    return pl.pallas_call(
        sink_kernel,
        in_specs=[hbm] * 4,
        out_specs=[vm] * 5 + [hbm],
        out_shape=[
            pltpu.VMEM((NDEV, 2 * ROWS, DIM), bf16),
            pltpu.VMEM((NDEV, 4, ROWS), f32),
            pltpu.VMEM((4, ROWS, 128), f32),
            pltpu.VMEM((2, KALL), f32),
            pltpu.VMEM((3, 128), f32),
            jax.ShapeDtypeStruct((2 * ROWS, KALL), f32),
        ],
        scratch_shapes=[
            pltpu.VMEM((2, NDEV, ROWS, DIM), bf16),
            pltpu.VMEM((NDEV, 1, ROWS), jnp.int32),
            pltpu.VMEM((KLOC, DIM), bf16),
            pltpu.VMEM((NS, NS), bf16),
            pltpu.VMEM((2, NS, DIM), bf16),
            pltpu.VMEM((2, KLOC, NS), f32),
            pltpu.VMEM((2, KLOC, NS), f32),
            pltpu.VMEM((2, KLOC, 128), f32),
            pltpu.VMEM((NDEV, 2, NS), f32),
            pltpu.VMEM((NDEV, 2, NS), f32),
            pltpu.VMEM((NDEV, 1, NS), f32),
            pltpu.VMEM((NDEV, 1, NS), f32),
            pltpu.VMEM((NDEV, 2, NS), f32),
            pltpu.VMEM((NDEV, 2, NS), f32),
            pltpu.VMEM((NDEV, 2, KLOC), f32),
            pltpu.VMEM((2 * ROWS, DIM), bf16),
            pltpu.VMEM((NBUF, PCH, DIM), bf16),
            pltpu.VMEM((NBUF, 2 * ROWS, PCH), f32),
            dma(()), dma((5,)),
            dma((7,)), dma((7,)),
            dma((2, 4)), dma((2, 4)),
            dma((2, 3)), dma((2, 3)),
            dma((6, 7)), dma((6, 7)),
            dma((7,)), dma((7,)),
            dma((NBUF,)), dma((NBUF,)),
        ],
        compiler_params=pltpu.CompilerParams(
            collective_id=0, has_side_effects=True, vmem_limit_bytes=VM1 * 1024 * 1024),
        name="sinkhorn",
    )(z1, z2, m, c)


def grad_kernel(c_ref, w_ref, vecs_ref, own_ref, b_ref, p_ref, stat_ref,
                q1_hbm, q2_hbm, dz1_ref, dz2_ref, dc_hbm, loss_ref,
                qbuf, dcbuf, bcol, q_sem, dc_sem):
    step = pl.program_id(0)
    last = KALL // TK - 1
    slot = lax.rem(step, 2)
    nck = TK // CK

    def q_store(st, v):
        sl = lax.rem(st, 2)
        return pltpu.make_async_copy(
            qbuf.at[sl, v], (q1_hbm, q2_hbm)[v].at[:, pl.ds(pl.multiple_of(st * TK, TK), TK)],
            q_sem.at[sl, v])

    def dc_store(st, k):
        sl = lax.rem(st, 2)
        return pltpu.make_async_copy(
            dcbuf.at[sl, pl.ds(k * CK, CK)],
            dc_hbm.at[pl.ds(pl.multiple_of(st * TK + k * CK, CK), CK), :], dc_sem.at[sl, k])

    @pl.when(step == 0)
    def _():
        dz1_ref[...] = jnp.zeros_like(dz1_ref)
        dz2_ref[...] = jnp.zeros_like(dz2_ref)
        loss_ref[...] = stat_ref[0:1, :]

    @pl.when(step >= 2)
    def _():
        for v in range(2):
            q_store(step - 2, v).wait()
        for k in range(nck):
            dc_store(step - 2, k).wait()

    koff = pl.multiple_of(step * TK, TK)
    g = stat_ref[1:2, 0:1]
    dz = jnp.zeros((2 * ROWS, DIM), jnp.float32)
    for t in range(TK // OS):
        cols = slice(t * OS, (t + 1) * OS)
        ps = [p_ref[:ROWS, cols], p_ref[ROWS:, cols]]
        qs = []
        for v in range(2):
            arow = jnp.concatenate([own_ref[v]] * (OS // 128), axis=1)
            q = (ps[v] * ps[v] * arow) * b_ref[v:v + 1, pl.ds(koff + t * OS, OS)]
            qbuf[slot, v, :, cols] = q
            qs.append(q)
        gs = []
        for v in range(2):
            al = jnp.concatenate([own_ref[2 + v]] * (OS // 128), axis=1)
            gs.append((ps[v] * al - qs[1 - v] * g).astype(jnp.bfloat16))
        dz = dz + dot_nn(jnp.concatenate(gs, axis=0), c_ref[cols, :])
    dz1_ref[...] += dz[:ROWS]
    dz2_ref[...] += dz[ROWS:]

    eye = (lax.broadcasted_iota(jnp.int32, (128, 128), 0)
           == lax.broadcasted_iota(jnp.int32, (128, 128), 1))
    for v in range(2):
        for t in range(TK // 128):
            blk = jnp.where(eye, jnp.broadcast_to(b_ref[v:v + 1, pl.ds(koff + t * 128, 128)], (128, 128)), 0.0)
            bcol[v, t * 128:(t + 1) * 128, :] = jnp.broadcast_to(
                jnp.sum(blk, axis=1, keepdims=True), (128, 128))

    tiles = (jnp.max(stat_ref[2:3, :]).astype(jnp.int32) + (ROWS - 1)) // ROWS

    def piece(t, idx):
        rows = slice(t * SUB, (t + 1) * SUB)
        w = w_ref[idx]
        vec = vecs_ref[idx]
        p = jnp.exp2(dot_nt(c_ref[rows, :], w) * C_EXP)
        p1, p2 = p[:, :ROWS], p[:, ROWS:]
        g1 = p1 * vec[0:1] - (p2 * p2 * bcol[1, rows, :]) * vec[3:4]
        g2 = p2 * vec[1:2] - (p1 * p1 * bcol[0, rows, :]) * vec[2:3]
        gg = jnp.concatenate([g1.astype(jnp.bfloat16), g2.astype(jnp.bfloat16)], axis=1)
        return dot_nn(gg, w)

    npc = TK // SUB

    def double(idx, flush):
        for t in range(npc):
            rows = slice(t * SUB, (t + 1) * SUB)
            dcbuf[slot, rows, :] += piece(t, idx) + piece(t, idx + 1)
            if flush and (t + 1) % (CK // SUB) == 0:
                dc_store(step, t // (CK // SUB)).start()

    for t in range(npc):
        dcbuf[slot, t * SUB:(t + 1) * SUB, :] = piece(t, 0) + piece(t, 1)
    for v in range(2):
        q_store(step, v).start()

    odd = tiles % 2
    pairs = (tiles - 2) // 2

    @pl.when(odd == 1)
    def _():
        for t in range(npc):
            dcbuf[slot, t * SUB:(t + 1) * SUB, :] += piece(t, 2)

    def body(i, carry):
        double(2 + odd + 2 * i, False)
        return carry
    lax.fori_loop(0, pairs - 1, body, 0)

    @pl.when(pairs >= 1)
    def _():
        double(tiles - 2, True)

    @pl.when(pairs < 1)
    def _():
        for k in range(nck):
            dc_store(step, k).start()

    @pl.when(step == last)
    def _():
        for st in (last - 1, last):
            for v in range(2):
                q_store(st, v).wait()
            for k in range(nck):
                dc_store(st, k).wait()


def grad_call(c, w, vecs, own, b, p, stat):
    f32, bf16 = jnp.float32, jnp.bfloat16
    whole = lambda shape: pl.BlockSpec(shape, lambda i: (0,) * len(shape))
    hbm = pl.BlockSpec(memory_space=pl.ANY)
    vm = pl.BlockSpec(memory_space=pltpu.VMEM)
    dma = pltpu.SemaphoreType.DMA
    return pl.pallas_call(
        grad_kernel,
        grid=(KALL // TK,),
        in_specs=[
            pl.BlockSpec((TK, DIM), lambda i: (i, 0)),
            vm, vm, vm,
            vm,
            pl.BlockSpec((2 * ROWS, TK), lambda i: (0, i)),
            vm,
        ],
        out_specs=[hbm, hbm, whole((ROWS, DIM)), whole((ROWS, DIM)), hbm, whole((1, 128))],
        out_shape=[
            jax.ShapeDtypeStruct((ROWS, KALL), f32),
            jax.ShapeDtypeStruct((ROWS, KALL), f32),
            jax.ShapeDtypeStruct((ROWS, DIM), f32),
            jax.ShapeDtypeStruct((ROWS, DIM), f32),
            jax.ShapeDtypeStruct((KALL, DIM), f32),
            jax.ShapeDtypeStruct((1, 128), f32),
        ],
        scratch_shapes=[
            pltpu.VMEM((2, 2, ROWS, TK), f32),
            pltpu.VMEM((2, TK, DIM), f32),
            pltpu.VMEM((2, TK, 128), f32),
            dma((2, 2)), dma((2, TK // CK)),
        ],
        compiler_params=pltpu.CompilerParams(vmem_limit_bytes=VM2 * 1024 * 1024),
        name="grads",
    )(c, w, vecs, own, b, p, stat)


def solution(mesh):
    def local_step(view_one, view_two, protos, valid_mask):
        w, vecs, own, b, stat, p = sink_call(
            view_one, view_two, valid_mask.reshape(1, ROWS), protos)
        q1, q2, dz1, dz2, dc, loss = grad_call(
            protos, w, vecs, own, b, p, stat)
        return q1, q2, loss[0, 0], dz1, dz2, dc

    return jax.shard_map(
        local_step,
        mesh=mesh,
        in_specs=(P("data", None), P("data", None), P(None, None), P("data")),
        out_specs=(P("data", None), P("data", None), P(), P("data", None), P("data", None), P(None, None)),
        check_vma=False,
    )
```

```python
import functools

import jax
import jax.numpy as jnp
from jax import lax
from jax.experimental import pallas as pl
from jax.experimental.pallas import tpu as pltpu
from jax.sharding import PartitionSpec as P

SOFT_TEMP = 0.1
LOG2E = 1.4426950408889634
C_EXP = LOG2E / SOFT_TEMP
MESH = pl.DeviceIdType.MESH
NDEV = 8
ROWS = 128
NS = NDEV * ROWS
DIM = 256
KALL = 16384
KLOC = KALL // NDEV
GRP = 128
CH = 256
TK = 4096
SUB = 256
CK = 1024
OS = 256

PCH = 1024
NPC = KALL // PCH
NBUF = 4
SPLIT = (10, 12, 14, 16)

VM1 = 56
VM2 = 50
NT_DIMS = (((1,), (1,)), ((), ()))


def dot_nt(x, y):
    return lax.dot_general(x, y, NT_DIMS, preferred_element_type=jnp.float32)


def dot_nn(x, y):
    return jnp.dot(x, y, preferred_element_type=jnp.float32)


def sink_kernel(z1_hbm, z2_hbm, m_hbm, c_hbm,
                w_ref, vecs_ref, own_ref, b_out, stat_ref, p_hbm,
                z_all, m_all, cs, ps, zcs, s_ref, e_ref, bcol,
                ar1, ar1b, ar2, ar2b, ar3, ar3b, b_all, zz, cbuf, pbuf,
                c_sem, in_sem, m_send, m_recv, z_send, z_recv, f_send, f_recv,
                ar_send, ar_recv, b_send, b_recv, cb_sem, pb_sem):
    me = lax.axis_index("data")
    chip, core = me // 2, me % 2
    partner = 2 * chip + (1 - core)
    peers = [lax.rem(me + o, NDEV) for o in range(1, NDEV)]
    same = [2 * lax.rem(chip + d, 4) + core for d in range(1, 4)]

    barrier = pltpu.get_barrier_semaphore()
    for peer in peers:
        pl.semaphore_signal(barrier, inc=1, device_id=(peer,), device_id_type=MESH)

    loads = [pltpu.make_async_copy(src, dst, in_sem.at[i]) for i, (src, dst) in enumerate((
        (z1_hbm, z_all.at[0, me]), (z2_hbm, z_all.at[1, me]), (m_hbm, m_all.at[me]),
        (z1_hbm, zz.at[pl.ds(0, ROWS)]), (z2_hbm, zz.at[pl.ds(ROWS, ROWS)])))]
    for cp in loads:
        cp.start()

    def c_load(j):
        return pltpu.make_async_copy(
            c_hbm.at[pl.ds(j * PCH, PCH), :], cbuf.at[j % NBUF], cb_sem.at[j % NBUF])

    def p_store(j):
        return pltpu.make_async_copy(
            pbuf.at[j % NBUF], p_hbm.at[:, pl.ds(j * PCH, PCH)], pb_sem.at[j % NBUF])

    for j in range(NBUF):
        c_load(j).start()
    cslice = pltpu.make_async_copy(c_hbm.at[pl.ds(me * KLOC, KLOC), :], cs, c_sem)
    cslice.start()

    def own_scores(lo, hi):
        for j in range(lo, hi):
            c_load(j).wait()
            if j >= NBUF:
                p_store(j - NBUF).wait()
            for t in range(PCH // 256):
                cols = slice(t * 256, (t + 1) * 256)
                sc = dot_nt(zz[...], cbuf[j % NBUF, cols, :])
                pbuf[j % NBUF, :, cols] = jnp.exp2(sc * C_EXP)
            p_store(j).start()
            if j + NBUF < NPC:
                c_load(j + NBUF).start()

    for cp in loads:
        cp.wait()
    pl.semaphore_wait(barrier, NDEV - 1)

    m_copies = []
    for o, peer in enumerate(peers):
        cp = pltpu.make_async_remote_copy(
            src_ref=m_all.at[me], dst_ref=m_all.at[me], send_sem=m_send.at[o],
            recv_sem=m_recv.at[o], device_id=(peer,), device_id_type=MESH)
        cp.start()
        m_copies.append(cp)
    z_copies = []
    for v in range(2):
        row = []
        for d, peer in enumerate(same + [partner]):
            cp = pltpu.make_async_remote_copy(
                src_ref=z_all.at[v, me], dst_ref=z_all.at[v, me], send_sem=z_send.at[v, d],
                recv_sem=z_recv.at[v, d], device_id=(peer,), device_id_type=MESH)
            cp.start()
            row.append(cp)
        z_copies.append(row)

    own_scores(0, SPLIT[0])
    for cp in m_copies:
        cp.wait_recv()
    mf = [jnp.broadcast_to(m_all[d].astype(jnp.float32), (8, ROWS)) for d in range(NDEV)]

    tri = (lax.broadcasted_iota(jnp.int32, (ROWS, ROWS), 0)
           < lax.broadcasted_iota(jnp.int32, (ROWS, ROWS), 1)).astype(jnp.bfloat16)
    base = jnp.zeros((8, 1), jnp.float32)
    pos_list = []
    for d in range(NDEV):
        md = mf[d]
        pre = dot_nn(md.astype(jnp.bfloat16), tri) + base
        pos_list.append(jnp.where(md > 0, pre, -1.0))
        base = base + jnp.sum(md, axis=1, keepdims=True)
    pos = jnp.concatenate(pos_list, axis=1)
    count = base
    mask = (lax.broadcasted_iota(jnp.int32, (8, NS), 1).astype(jnp.float32) < count)
    maskf = mask.astype(jnp.float32)
    for t in range(NS // 128):
        idx = (lax.broadcasted_iota(jnp.int32, (128, NS), 0) + t * 128).astype(jnp.float32)
        ps[t * 128:(t + 1) * 128, :] = (jnp.broadcast_to(pos[0:1], (128, NS)) == idx).astype(jnp.bfloat16)

    def forward(v):
        out = []
        for d in range(3):
            z_copies[v][d].wait_recv()
            frm = 2 * lax.rem(chip + 3 - d, 4) + core
            cp = pltpu.make_async_remote_copy(
                src_ref=z_all.at[v, frm], dst_ref=z_all.at[v, frm], send_sem=f_send.at[v, d],
                recv_sem=f_recv.at[v, d], device_id=(partner,), device_id_type=MESH)
            cp.start()
            out.append(cp)
        return out

    def compact(v, fw):
        z_copies[v][3].wait_recv()
        for cp in fw:
            cp.wait_recv()
        zv = z_all[v].reshape(NS, DIM)
        for t in range(NS // 256):
            rows = slice(t * 256, (t + 1) * 256)
            zc = dot_nn(ps[rows, :], zv).astype(jnp.bfloat16)
            zcs[v, rows, :] = zc
            w_ref[2 * t, v * ROWS:(v + 1) * ROWS, :] = zc[:ROWS]
            w_ref[2 * t + 1, v * ROWS:(v + 1) * ROWS, :] = zc[ROWS:]

    def exchange(idx, buf):
        copies = []
        for o, peer in enumerate(peers):
            cp = pltpu.make_async_remote_copy(
                src_ref=buf.at[me], dst_ref=buf.at[me], send_sem=ar_send.at[idx, o],
                recv_sem=ar_recv.at[idx, o], device_id=(peer,), device_id_type=MESH)
            cp.start()
            copies.append(cp)
        return copies

    def total(buf, copies):
        for cp in copies:
            cp.wait_recv()
        acc = buf[0]
        for d in range(1, NDEV):
            acc = acc + buf[d]
        return acc

    def rsum(x):
        return jnp.sum(x, axis=0, keepdims=True)

    m1 = maskf[0:1]

    def recip(r):
        return jnp.where(m1 > 0, 1.0 / jnp.where(m1 > 0, r, 1.0), 0.0)

    zero = jnp.zeros((8, NS), jnp.float32)

    def first_pass(v, lo, hi, carry):
        racc, lacc = carry

        def rows_part(i, racc):
            for g in range(CH // 8):
                rows = slice(i * CH + g * 8, i * CH + g * 8 + 8)
                b = jnp.concatenate([bcol[v, rows, :]] * (NS // 128), axis=1)
                racc = racc + e_ref[v, rows, :] * b
            return racc

        for i in range(lo, hi):
            off = i * CH
            s_ref[v, off:off + CH, :] = dot_nt(cs[off:off + CH, :], zcs[v])
            for g in range(CH // 8):
                rows = slice(off + g * 8, off + g * 8 + 8)
                p = jnp.exp2(s_ref[v, rows, :] * C_EXP)
                lacc = lacc + p
                e = p * p * maskf
                e_ref[v, rows, :] = e
                bcol[v, rows, :] = jnp.broadcast_to(1.0 / jnp.sum(e, axis=1, keepdims=True), (8, 128))
            if i > lo:
                racc = rows_part(i - 1, racc)
        return rows_part(hi - 1, racc), lacc

    def sweep(v, a, last):
        a8 = jnp.broadcast_to(a, (8, NS))

        def body(i, carry):
            carry = list(carry)
            off = pl.multiple_of(i * (GRP * 8), GRP * 8)
            for g in range(GRP):
                rows = pl.ds(off + g * 8, 8)
                e = e_ref[v, rows, :]
                b = 1.0 / jnp.sum(e * a8, axis=1, keepdims=True)
                eb = e * b
                carry[0] = carry[0] + eb
                if last:
                    bcol[v, rows, :] = jnp.broadcast_to(b, (8, 128))
                    carry[1] = carry[1] + eb * s_ref[1 - v, rows, :]
            return tuple(carry)
        return lax.fori_loop(0, KLOC // (GRP * 8), body, (zero,) * (2 if last else 1))

    half = KLOC // CH // 2
    fw1 = forward(0)
    own_scores(SPLIT[0], SPLIT[1])
    cslice.wait()
    compact(0, fw1)
    acc = first_pass(0, 0, half, (zero, zero))
    fw2 = forward(1)
    racc, lacc = first_pass(0, half, 2 * half, acc)
    ar1[me, 0:1, :] = rsum(racc)
    ar1[me, 1:2, :] = rsum(lacc)
    x1 = [exchange(0, ar1)]
    compact(1, fw2)
    racc, lacc = first_pass(1, 0, 2 * half, (zero, zero))
    ar1b[me, 0:1, :] = rsum(racc)
    ar1b[me, 1:2, :] = rsum(lacc)
    x1.append(exchange(1, ar1b))

    lse, x2 = [], []
    for v, (b1, b2) in enumerate(((ar1, ar2), (ar1b, ar2b))):
        if v == 1:
            own_scores(SPLIT[1], SPLIT[2])
        tot = total(b1, x1[v])
        lse.append(tot[1:2])
        r, = sweep(v, recip(tot[0:1]), False)
        b2[me] = rsum(r)
        x2.append(exchange(2 + v, b2))

    x3, b_copies = [], []
    eye = (lax.broadcasted_iota(jnp.int32, (128, 128), 0)
           == lax.broadcasted_iota(jnp.int32, (128, 128), 1))
    for v, (b2, b3) in enumerate(((ar2, ar3), (ar2b, ar3b))):
        if v == 1:
            own_scores(SPLIT[2], SPLIT[3])
        tot = total(b2, x2[v])
        r, tl = sweep(v, recip(tot), True)
        b3[me, 0:1, :] = rsum(r)
        b3[me, 1:2, :] = rsum(tl)
        x3.append(exchange(4 + v, b3))
        for t in range(KLOC // 128):
            blk = bcol[v, t * 128:(t + 1) * 128, :]
            b_all[me, v:v + 1, t * 128:(t + 1) * 128] = jnp.sum(
                jnp.where(eye, blk, 0.0), axis=0, keepdims=True)
    for o, peer in enumerate(peers):
        cp = pltpu.make_async_remote_copy(
            src_ref=b_all.at[me], dst_ref=b_all.at[me], send_sem=b_send.at[o],
            recv_sem=b_recv.at[o], device_id=(peer,), device_id_type=MESH)
        cp.start()
        b_copies.append(cp)

    cnt = count[0:1]
    g = 1.0 / (2.0 * SOFT_TEMP * cnt)
    alpha = [m1 * g / x for x in lse]
    stat_ref[1:2, :] = jnp.broadcast_to(g, (1, 128))
    stat_ref[2:3, :] = jnp.broadcast_to(cnt, (1, 128))
    before = jnp.zeros((1, 1), jnp.float32)
    for d in range(NDEV):
        before = before + jnp.where(d < me, 1.0, 0.0) * jnp.sum(mf[d][0:1], axis=1, keepdims=True)
    mine = jnp.broadcast_to(m_all[me].astype(jnp.float32), (8, ROWS))
    pre = dot_nn(mine.astype(jnp.bfloat16), tri)[0:1] + before
    pre = jnp.where(mine[0:1] > 0, pre, -1.0)
    pcol = jnp.sum(jnp.where(eye, jnp.broadcast_to(pre, (128, 128)), 0.0), axis=1, keepdims=True)
    lane = lax.broadcasted_iota(jnp.int32, (128, NS), 1).astype(jnp.float32)
    hit = lane == pcol

    def put(i, x, scale):
        col = jnp.sum(jnp.where(hit, jnp.broadcast_to(x, (128, NS)), 0.0), axis=1, keepdims=True)
        own_ref[i] = jnp.broadcast_to(col, (128, 128))
        y = x * scale
        for t in range(NDEV):
            j = (i + 2) % 4
            vecs_ref[t, j:j + 1, :] = y[:, t * 128:(t + 1) * 128]

    put(2, alpha[0], 1.0)
    put(3, alpha[1], 1.0)
    own_scores(SPLIT[3], NPC)

    tots = [total(ar3, x3[0])]
    a0 = recip(tots[0][0:1])
    put(0, a0, g)
    tots.append(total(ar3b, x3[1]))
    a1 = recip(tots[1][0:1])
    put(1, a1, g)
    inner = sum(a * (tots[v][1:2] * (1.0 / SOFT_TEMP)) - a * tots[v][0:1] * jnp.log(lse[1 - v])
                for v, a in enumerate((a0, a1)))
    loss = -jnp.sum(jnp.where(m1 > 0, inner, 0.0), axis=1, keepdims=True) / (2.0 * cnt)
    stat_ref[0:1, :] = jnp.broadcast_to(loss, (1, 128))

    for cp in b_copies:
        cp.wait_recv()
    for d in range(NDEV):
        lo_col = d * KLOC
        b_out[lo_col // TK, :, lo_col % TK:lo_col % TK + KLOC] = b_all[d]
    for j in range(NPC - NBUF, NPC):
        p_store(j).wait()
    for cp in m_copies + z_copies[0] + z_copies[1] + fw1 + fw2 + sum(x1 + x2 + x3, []) + b_copies:
        cp.wait_send()


def sink_call(z1, z2, m, c):
    f32, bf16 = jnp.float32, jnp.bfloat16
    vm = pl.BlockSpec(memory_space=pltpu.VMEM)
    hbm = pl.BlockSpec(memory_space=pltpu.HBM)
    dma = pltpu.SemaphoreType.DMA
    return pl.pallas_call(
        sink_kernel,
        in_specs=[hbm] * 4,
        out_specs=[vm] * 5 + [hbm],
        out_shape=[
            pltpu.VMEM((NDEV, 2 * ROWS, DIM), bf16),
            pltpu.VMEM((NDEV, 4, ROWS), f32),
            pltpu.VMEM((4, ROWS, 128), f32),
            pltpu.VMEM((KALL // TK, 2, TK), f32),
            pltpu.VMEM((3, 128), f32),
            jax.ShapeDtypeStruct((2 * ROWS, KALL), f32),
        ],
        scratch_shapes=[
            pltpu.VMEM((2, NDEV, ROWS, DIM), bf16),
            pltpu.VMEM((NDEV, 1, ROWS), jnp.int32),
            pltpu.VMEM((KLOC, DIM), bf16),
            pltpu.VMEM((NS, NS), bf16),
            pltpu.VMEM((2, NS, DIM), bf16),
            pltpu.VMEM((2, KLOC, NS), f32),
            pltpu.VMEM((2, KLOC, NS), f32),
            pltpu.VMEM((2, KLOC, 128), f32),
            pltpu.VMEM((NDEV, 2, NS), f32),
            pltpu.VMEM((NDEV, 2, NS), f32),
            pltpu.VMEM((NDEV, 1, NS), f32),
            pltpu.VMEM((NDEV, 1, NS), f32),
            pltpu.VMEM((NDEV, 2, NS), f32),
            pltpu.VMEM((NDEV, 2, NS), f32),
            pltpu.VMEM((NDEV, 2, KLOC), f32),
            pltpu.VMEM((2 * ROWS, DIM), bf16),
            pltpu.VMEM((NBUF, PCH, DIM), bf16),
            pltpu.VMEM((NBUF, 2 * ROWS, PCH), f32),
            dma(()), dma((5,)),
            dma((7,)), dma((7,)),
            dma((2, 4)), dma((2, 4)),
            dma((2, 3)), dma((2, 3)),
            dma((6, 7)), dma((6, 7)),
            dma((7,)), dma((7,)),
            dma((NBUF,)), dma((NBUF,)),
        ],
        compiler_params=pltpu.CompilerParams(
            collective_id=0, has_side_effects=True, vmem_limit_bytes=VM1 * 1024 * 1024),
        name="sinkhorn",
    )(z1, z2, m, c)


def grad_kernel(c_ref, w_ref, vecs_ref, own_ref, b_ref, p_ref, stat_ref,
                q1_hbm, q2_hbm, dz1_ref, dz2_ref, dc_hbm, loss_ref,
                qbuf, dcbuf, bcol, q_sem, dc_sem):
    step = pl.program_id(0)
    last = KALL // TK - 1
    slot = lax.rem(step, 2)
    nck = TK // CK

    def q_store(st, v):
        sl = lax.rem(st, 2)
        return pltpu.make_async_copy(
            qbuf.at[sl, v], (q1_hbm, q2_hbm)[v].at[:, pl.ds(pl.multiple_of(st * TK, TK), TK)],
            q_sem.at[sl, v])

    def dc_store(st, k):
        sl = lax.rem(st, 2)
        return pltpu.make_async_copy(
            dcbuf.at[sl, pl.ds(k * CK, CK)],
            dc_hbm.at[pl.ds(pl.multiple_of(st * TK + k * CK, CK), CK), :], dc_sem.at[sl, k])

    @pl.when(step == 0)
    def _():
        dz1_ref[...] = jnp.zeros_like(dz1_ref)
        dz2_ref[...] = jnp.zeros_like(dz2_ref)
        loss_ref[...] = stat_ref[0:1, :]

    @pl.when(step >= 2)
    def _():
        for v in range(2):
            q_store(step - 2, v).wait()
        for k in range(nck):
            dc_store(step - 2, k).wait()

    g = stat_ref[1:2, 0:1]
    dz = jnp.zeros((2 * ROWS, DIM), jnp.float32)
    for t in range(TK // OS):
        cols = slice(t * OS, (t + 1) * OS)
        ps = [p_ref[:ROWS, cols], p_ref[ROWS:, cols]]
        qs = []
        for v in range(2):
            arow = jnp.concatenate([own_ref[v]] * (OS // 128), axis=1)
            q = (ps[v] * ps[v] * arow) * b_ref[step, v:v + 1, cols]
            qbuf[slot, v, :, cols] = q
            qs.append(q)
        gs = []
        for v in range(2):
            al = jnp.concatenate([own_ref[2 + v]] * (OS // 128), axis=1)
            gs.append((ps[v] * al - qs[1 - v] * g).astype(jnp.bfloat16))
        dz = dz + dot_nn(jnp.concatenate(gs, axis=0), c_ref[cols, :])
    dz1_ref[...] += dz[:ROWS]
    dz2_ref[...] += dz[ROWS:]

    for v in range(2):
        for t in range(TK // 128):
            blk = jnp.broadcast_to(b_ref[step, v:v + 1, t * 128:(t + 1) * 128], (128, 128))
            bcol[v, t * 128:(t + 1) * 128, :] = jnp.transpose(blk)

    tiles = (jnp.max(stat_ref[2:3, :]).astype(jnp.int32) + (ROWS - 1)) // ROWS

    def piece(t, idx):
        rows = slice(t * SUB, (t + 1) * SUB)
        w = w_ref[idx]
        vec = vecs_ref[idx]
        p = jnp.exp2(dot_nt(c_ref[rows, :], w) * C_EXP)
        p1, p2 = p[:, :ROWS], p[:, ROWS:]
        g1 = p1 * vec[0:1] - (p2 * p2 * bcol[1, rows, :]) * vec[3:4]
        g2 = p2 * vec[1:2] - (p1 * p1 * bcol[0, rows, :]) * vec[2:3]
        gg = jnp.concatenate([g1.astype(jnp.bfloat16), g2.astype(jnp.bfloat16)], axis=1)
        return dot_nn(gg, w)

    npc = TK // SUB

    def add_tiles(idx, n, flush):
        for t in range(npc):
            rows = slice(t * SUB, (t + 1) * SUB)
            dcbuf[slot, rows, :] += sum(piece(t, idx + i) for i in range(n))
            if flush and (t + 1) % (CK // SUB) == 0:
                dc_store(step, t // (CK // SUB)).start()

    for t in range(npc):
        dcbuf[slot, t * SUB:(t + 1) * SUB, :] = piece(t, 0) + piece(t, 1)
    for v in range(2):
        q_store(step, v).start()

    rest = tiles - 2
    fin = jnp.where(rest == 1, 1, jnp.where(rest % 2 == 1, 3, jnp.minimum(rest, 2)))

    def body(i, carry):
        add_tiles(2 + 2 * i, 2, False)
        return carry
    lax.fori_loop(0, (rest - fin) // 2, body, 0)

    for n in (1, 2, 3):
        @pl.when(fin == n)
        def _(n=n):
            add_tiles(tiles - n, n, True)

    @pl.when(fin == 0)
    def _():
        for k in range(nck):
            dc_store(step, k).start()

    @pl.when(step == last)
    def _():
        for st in (last - 1, last):
            for v in range(2):
                q_store(st, v).wait()
            for k in range(nck):
                dc_store(st, k).wait()


def grad_call(c, w, vecs, own, b, p, stat):
    f32, bf16 = jnp.float32, jnp.bfloat16
    whole = lambda shape: pl.BlockSpec(shape, lambda i: (0,) * len(shape))
    hbm = pl.BlockSpec(memory_space=pl.ANY)
    vm = pl.BlockSpec(memory_space=pltpu.VMEM)
    dma = pltpu.SemaphoreType.DMA
    return pl.pallas_call(
        grad_kernel,
        grid=(KALL // TK,),
        in_specs=[
            pl.BlockSpec((TK, DIM), lambda i: (i, 0)),
            vm, vm, vm,
            vm,
            pl.BlockSpec((2 * ROWS, TK), lambda i: (0, i)),
            vm,
        ],
        out_specs=[hbm, hbm, whole((ROWS, DIM)), whole((ROWS, DIM)), hbm, whole((1, 128))],
        out_shape=[
            jax.ShapeDtypeStruct((ROWS, KALL), f32),
            jax.ShapeDtypeStruct((ROWS, KALL), f32),
            jax.ShapeDtypeStruct((ROWS, DIM), f32),
            jax.ShapeDtypeStruct((ROWS, DIM), f32),
            jax.ShapeDtypeStruct((KALL, DIM), f32),
            jax.ShapeDtypeStruct((1, 128), f32),
        ],
        scratch_shapes=[
            pltpu.VMEM((2, 2, ROWS, TK), f32),
            pltpu.VMEM((2, TK, DIM), f32),
            pltpu.VMEM((2, TK, 128), f32),
            dma((2, 2)), dma((2, TK // CK)),
        ],
        compiler_params=pltpu.CompilerParams(vmem_limit_bytes=VM2 * 1024 * 1024),
        name="grads",
    )(c, w, vecs, own, b, p, stat)


def solution(mesh):
    def local_step(view_one, view_two, protos, valid_mask):
        w, vecs, own, b, stat, p = sink_call(
            view_one, view_two, valid_mask.reshape(1, ROWS), protos)
        q1, q2, dz1, dz2, dc, loss = grad_call(
            protos, w, vecs, own, b, p, stat)
        return q1, q2, loss[0, 0], dz1, dz2, dc

    return jax.shard_map(
        local_step,
        mesh=mesh,
        in_specs=(P("data", None), P("data", None), P(None, None), P("data")),
        out_specs=(P("data", None), P("data", None), P(), P("data", None), P("data", None), P(None, None)),
        check_vma=False,
    )
```

```python
import functools

import jax
import jax.numpy as jnp
from jax import lax
from jax.experimental import pallas as pl
from jax.experimental.pallas import tpu as pltpu
from jax.sharding import PartitionSpec as P

SOFT_TEMP = 0.1
LOG2E = 1.4426950408889634
C_EXP = LOG2E / SOFT_TEMP
MESH = pl.DeviceIdType.MESH
NDEV = 8
ROWS = 128
NS = NDEV * ROWS
DIM = 256
KALL = 16384
KLOC = KALL // NDEV
GRP = 128
CH = 256
TK = 4096
SUB = 512
CK = 1024
OS = 256

PCH = 1024
NPC = KALL // PCH
NBUF = 4
SPLIT = (10, 12, 14, 16)

VM1 = 54
VM2 = 47
NT_DIMS = (((1,), (1,)), ((), ()))


def dot_nt(x, y):
    return lax.dot_general(x, y, NT_DIMS, preferred_element_type=jnp.float32)


def dot_nn(x, y):
    return jnp.dot(x, y, preferred_element_type=jnp.float32)


def sink_kernel(z1_hbm, z2_hbm, m_hbm, c_hbm,
                w_ref, vecs_ref, own_ref, b_out, stat_ref, p0_out, p_hbm,
                z_all, m_all, cs, ps, zcs, s_ref, e_ref, bcol,
                ar1, ar1b, ar2, ar2b, ar3, ar3b, b_all, zz, cbuf, pbuf,
                c_sem, in_sem, m_send, m_recv, z_send, z_recv, f_send, f_recv,
                ar_send, ar_recv, b_send, b_recv, cb_sem, pb_sem):
    me = lax.axis_index("data")
    chip, core = me // 2, me % 2
    partner = 2 * chip + (1 - core)
    peers = [lax.rem(me + o, NDEV) for o in range(1, NDEV)]
    same = [2 * lax.rem(chip + d, 4) + core for d in range(1, 4)]

    barrier = pltpu.get_barrier_semaphore()
    for peer in peers:
        pl.semaphore_signal(barrier, inc=1, device_id=(peer,), device_id_type=MESH)

    loads = [pltpu.make_async_copy(src, dst, in_sem.at[i]) for i, (src, dst) in enumerate((
        (z1_hbm, z_all.at[0, me]), (z2_hbm, z_all.at[1, me]), (m_hbm, m_all.at[me]),
        (z1_hbm, zz.at[pl.ds(0, ROWS)]), (z2_hbm, zz.at[pl.ds(ROWS, ROWS)])))]
    for cp in loads:
        cp.start()

    def c_load(j):
        return pltpu.make_async_copy(
            c_hbm.at[pl.ds(j * PCH, PCH), :], cbuf.at[j % NBUF], cb_sem.at[j % NBUF])

    def p_store(j):
        return pltpu.make_async_copy(
            pbuf.at[j % NBUF], p_hbm.at[:, pl.ds(j * PCH - TK, PCH)], pb_sem.at[j % NBUF])

    for j in range(NBUF):
        c_load(j).start()
    cslice = pltpu.make_async_copy(c_hbm.at[pl.ds(me * KLOC, KLOC), :], cs, c_sem)
    cslice.start()

    def own_scores(lo, hi):
        for j in range(lo, hi):
            c_load(j).wait()
            if j - NBUF >= TK // PCH:
                p_store(j - NBUF).wait()
            for t in range(PCH // 256):
                cols = slice(t * 256, (t + 1) * 256)
                sc = dot_nt(zz[...], cbuf[j % NBUF, cols, :])
                if j < TK // PCH:
                    p0_out[:, j * PCH + t * 256:j * PCH + (t + 1) * 256] = jnp.exp2(sc * C_EXP)
                else:
                    pbuf[j % NBUF, :, cols] = jnp.exp2(sc * C_EXP)
            if j >= TK // PCH:
                p_store(j).start()
            if j + NBUF < NPC:
                c_load(j + NBUF).start()

    for cp in loads:
        cp.wait()
    pl.semaphore_wait(barrier, NDEV - 1)

    m_copies = []
    for o, peer in enumerate(peers):
        cp = pltpu.make_async_remote_copy(
            src_ref=m_all.at[me], dst_ref=m_all.at[me], send_sem=m_send.at[o],
            recv_sem=m_recv.at[o], device_id=(peer,), device_id_type=MESH)
        cp.start()
        m_copies.append(cp)
    z_copies = []
    for v in range(2):
        row = []
        for d, peer in enumerate(same + [partner]):
            cp = pltpu.make_async_remote_copy(
                src_ref=z_all.at[v, me], dst_ref=z_all.at[v, me], send_sem=z_send.at[v, d],
                recv_sem=z_recv.at[v, d], device_id=(peer,), device_id_type=MESH)
            cp.start()
            row.append(cp)
        z_copies.append(row)

    own_scores(0, SPLIT[0])
    for cp in m_copies:
        cp.wait_recv()
    mf = [jnp.broadcast_to(m_all[d].astype(jnp.float32), (8, ROWS)) for d in range(NDEV)]

    tri = (lax.broadcasted_iota(jnp.int32, (ROWS, ROWS), 0)
           < lax.broadcasted_iota(jnp.int32, (ROWS, ROWS), 1)).astype(jnp.bfloat16)
    base = jnp.zeros((8, 1), jnp.float32)
    pos_list = []
    for d in range(NDEV):
        md = mf[d]
        pre = dot_nn(md.astype(jnp.bfloat16), tri) + base
        pos_list.append(jnp.where(md > 0, pre, -1.0))
        base = base + jnp.sum(md, axis=1, keepdims=True)
    pos = jnp.concatenate(pos_list, axis=1)
    count = base
    mask = (lax.broadcasted_iota(jnp.int32, (8, NS), 1).astype(jnp.float32) < count)
    maskf = mask.astype(jnp.float32)
    for t in range(NS // 128):
        lo_col = t // 2 * 256
        idx = (lax.broadcasted_iota(jnp.int32, (128, NS - lo_col), 0) + t * 128).astype(jnp.float32)
        ps[t * 128:(t + 1) * 128, lo_col:] = (
            jnp.broadcast_to(pos[0:1, lo_col:], (128, NS - lo_col)) == idx).astype(jnp.bfloat16)

    def forward(v):
        out = []
        for d in range(3):
            z_copies[v][d].wait_recv()
            frm = 2 * lax.rem(chip + 3 - d, 4) + core
            cp = pltpu.make_async_remote_copy(
                src_ref=z_all.at[v, frm], dst_ref=z_all.at[v, frm], send_sem=f_send.at[v, d],
                recv_sem=f_recv.at[v, d], device_id=(partner,), device_id_type=MESH)
            cp.start()
            out.append(cp)
        return out

    def compact(v, fw):
        z_copies[v][3].wait_recv()
        for cp in fw:
            cp.wait_recv()
        zv = z_all[v].reshape(NS, DIM)
        for t in range(NS // 256):
            rows = slice(t * 256, (t + 1) * 256)
            zc = dot_nn(ps[rows, t * 256:], zv[t * 256:]).astype(jnp.bfloat16)
            zcs[v, rows, :] = zc
            w_ref[2 * t, v * ROWS:(v + 1) * ROWS, :] = zc[:ROWS]
            w_ref[2 * t + 1, v * ROWS:(v + 1) * ROWS, :] = zc[ROWS:]

    def exchange(idx, buf):
        copies = []
        for o, peer in enumerate(peers):
            cp = pltpu.make_async_remote_copy(
                src_ref=buf.at[me], dst_ref=buf.at[me], send_sem=ar_send.at[idx, o],
                recv_sem=ar_recv.at[idx, o], device_id=(peer,), device_id_type=MESH)
            cp.start()
            copies.append(cp)
        return copies

    def total(buf, copies):
        for cp in copies:
            cp.wait_recv()
        acc = buf[0]
        for d in range(1, NDEV):
            acc = acc + buf[d]
        return acc

    def rsum(x):
        return jnp.sum(x, axis=0, keepdims=True)

    m1 = maskf[0:1]

    def recip(r):
        return jnp.where(m1 > 0, 1.0 / jnp.where(m1 > 0, r, 1.0), 0.0)

    zero = jnp.zeros((8, NS), jnp.float32)

    def first_pass(v, lo, hi, carry):
        racc, lacc = carry

        def rows_part(i, racc):
            for g in range(CH // 8):
                rows = slice(i * CH + g * 8, i * CH + g * 8 + 8)
                b = jnp.concatenate([bcol[v, rows, :]] * (NS // 128), axis=1)
                racc = racc + e_ref[v, rows, :] * b
            return racc

        for i in range(lo, hi):
            off = i * CH
            s_ref[v, off:off + CH, :] = dot_nt(cs[off:off + CH, :], zcs[v])
            for g in range(CH // 8):
                rows = slice(off + g * 8, off + g * 8 + 8)
                p = jnp.exp2(s_ref[v, rows, :] * C_EXP)
                lacc = lacc + p
                e = p * p * maskf
                e_ref[v, rows, :] = e
                bcol[v, rows, :] = jnp.broadcast_to(1.0 / jnp.sum(e, axis=1, keepdims=True), (8, 128))
            if i > lo:
                racc = rows_part(i - 1, racc)
        return rows_part(hi - 1, racc), lacc

    def sweep(v, a, last):
        a8 = jnp.broadcast_to(a, (8, NS))

        def body(i, carry):
            carry = list(carry)
            off = pl.multiple_of(i * (GRP * 8), GRP * 8)
            for g in range(GRP):
                rows = pl.ds(off + g * 8, 8)
                e = e_ref[v, rows, :]
                b = 1.0 / jnp.sum(e * a8, axis=1, keepdims=True)
                eb = e * b
                carry[0] = carry[0] + eb
                if last:
                    bcol[v, rows, :] = jnp.broadcast_to(b, (8, 128))
                    carry[1] = carry[1] + eb * s_ref[1 - v, rows, :]
            return tuple(carry)
        return lax.fori_loop(0, KLOC // (GRP * 8), body, (zero,) * (2 if last else 1))

    half = KLOC // CH // 2
    fw1 = forward(0)
    own_scores(SPLIT[0], SPLIT[1])
    cslice.wait()
    compact(0, fw1)
    acc = first_pass(0, 0, half, (zero, zero))
    fw2 = forward(1)
    racc, lacc = first_pass(0, half, 2 * half, acc)
    ar1[me, 0:1, :] = rsum(racc)
    ar1[me, 1:2, :] = rsum(lacc)
    x1 = [exchange(0, ar1)]
    compact(1, fw2)
    racc, lacc = first_pass(1, 0, 2 * half, (zero, zero))
    ar1b[me, 0:1, :] = rsum(racc)
    ar1b[me, 1:2, :] = rsum(lacc)
    x1.append(exchange(1, ar1b))

    lse, x2 = [], []
    for v, (b1, b2) in enumerate(((ar1, ar2), (ar1b, ar2b))):
        if v == 1:
            own_scores(SPLIT[1], SPLIT[2])
        tot = total(b1, x1[v])
        lse.append(tot[1:2])
        r, = sweep(v, recip(tot[0:1]), False)
        b2[me] = rsum(r)
        x2.append(exchange(2 + v, b2))

    x3, b_copies = [], []
    eye = (lax.broadcasted_iota(jnp.int32, (128, 128), 0)
           == lax.broadcasted_iota(jnp.int32, (128, 128), 1))
    for v, (b2, b3) in enumerate(((ar2, ar3), (ar2b, ar3b))):
        if v == 1:
            own_scores(SPLIT[2], SPLIT[3])
        tot = total(b2, x2[v])
        r, tl = sweep(v, recip(tot), True)
        b3[me, 0:1, :] = rsum(r)
        b3[me, 1:2, :] = rsum(tl)
        x3.append(exchange(4 + v, b3))
        for t in range(KLOC // 128):
            blk = bcol[v, t * 128:(t + 1) * 128, :]
            b_all[me, v:v + 1, t * 128:(t + 1) * 128] = jnp.sum(
                jnp.where(eye, blk, 0.0), axis=0, keepdims=True)
    for o, peer in enumerate(peers):
        cp = pltpu.make_async_remote_copy(
            src_ref=b_all.at[me], dst_ref=b_all.at[me], send_sem=b_send.at[o],
            recv_sem=b_recv.at[o], device_id=(peer,), device_id_type=MESH)
        cp.start()
        b_copies.append(cp)

    cnt = count[0:1]
    g = 1.0 / (2.0 * SOFT_TEMP * cnt)
    alpha = [m1 * g / x for x in lse]
    stat_ref[1:2, :] = jnp.broadcast_to(g, (1, 128))
    stat_ref[2:3, :] = jnp.broadcast_to(cnt, (1, 128))
    before = jnp.zeros((1, 1), jnp.float32)
    for d in range(NDEV):
        before = before + jnp.where(d < me, 1.0, 0.0) * jnp.sum(mf[d][0:1], axis=1, keepdims=True)
    mine = jnp.broadcast_to(m_all[me].astype(jnp.float32), (8, ROWS))
    pre = dot_nn(mine.astype(jnp.bfloat16), tri)[0:1] + before
    pre = jnp.where(mine[0:1] > 0, pre, -1.0)
    pcol = jnp.sum(jnp.where(eye, jnp.broadcast_to(pre, (128, 128)), 0.0), axis=1, keepdims=True)
    lane = lax.broadcasted_iota(jnp.int32, (128, NS), 1).astype(jnp.float32)
    hit = lane == pcol

    def put(i, x, scale):
        col = jnp.sum(jnp.where(hit, jnp.broadcast_to(x, (128, NS)), 0.0), axis=1, keepdims=True)
        own_ref[i] = jnp.broadcast_to(col, (128, 128))
        y = x * scale
        for t in range(NDEV):
            j = (i + 2) % 4
            vecs_ref[t, j:j + 1, :] = y[:, t * 128:(t + 1) * 128]

    put(2, alpha[0], 1.0)
    put(3, alpha[1], 1.0)
    own_scores(SPLIT[3], NPC)

    tots = [total(ar3, x3[0])]
    a0 = recip(tots[0][0:1])
    put(0, a0, g)
    tots.append(total(ar3b, x3[1]))
    a1 = recip(tots[1][0:1])
    put(1, a1, g)
    inner = sum(a * (tots[v][1:2] * (1.0 / SOFT_TEMP)) - a * tots[v][0:1] * jnp.log(lse[1 - v])
                for v, a in enumerate((a0, a1)))
    loss = -jnp.sum(jnp.where(m1 > 0, inner, 0.0), axis=1, keepdims=True) / (2.0 * cnt)
    stat_ref[0:1, :] = jnp.broadcast_to(loss, (1, 128))

    for cp in b_copies:
        cp.wait_recv()
    for d in range(NDEV):
        lo_col = d * KLOC
        b_out[lo_col // TK, :, lo_col % TK:lo_col % TK + KLOC] = b_all[d]
    for j in range(NPC - NBUF, NPC):
        p_store(j).wait()
    for cp in m_copies + z_copies[0] + z_copies[1] + fw1 + fw2 + sum(x1 + x2 + x3, []) + b_copies:
        cp.wait_send()


def sink_call(z1, z2, m, c):
    f32, bf16 = jnp.float32, jnp.bfloat16
    vm = pl.BlockSpec(memory_space=pltpu.VMEM)
    hbm = pl.BlockSpec(memory_space=pltpu.HBM)
    dma = pltpu.SemaphoreType.DMA
    return pl.pallas_call(
        sink_kernel,
        in_specs=[hbm] * 4,
        out_specs=[vm] * 6 + [hbm],
        out_shape=[
            pltpu.VMEM((NDEV, 2 * ROWS, DIM), bf16),
            pltpu.VMEM((NDEV, 4, ROWS), f32),
            pltpu.VMEM((4, ROWS, 128), f32),
            pltpu.VMEM((KALL // TK, 2, TK), f32),
            pltpu.VMEM((3, 128), f32),
            pltpu.VMEM((2 * ROWS, TK), f32),
            jax.ShapeDtypeStruct((2 * ROWS, KALL - TK), f32),
        ],
        scratch_shapes=[
            pltpu.VMEM((2, NDEV, ROWS, DIM), bf16),
            pltpu.VMEM((NDEV, 1, ROWS), jnp.int32),
            pltpu.VMEM((KLOC, DIM), bf16),
            pltpu.VMEM((NS, NS), bf16),
            pltpu.VMEM((2, NS, DIM), bf16),
            pltpu.VMEM((2, KLOC, NS), f32),
            pltpu.VMEM((2, KLOC, NS), f32),
            pltpu.VMEM((2, KLOC, 128), f32),
            pltpu.VMEM((NDEV, 2, NS), f32),
            pltpu.VMEM((NDEV, 2, NS), f32),
            pltpu.VMEM((NDEV, 1, NS), f32),
            pltpu.VMEM((NDEV, 1, NS), f32),
            pltpu.VMEM((NDEV, 2, NS), f32),
            pltpu.VMEM((NDEV, 2, NS), f32),
            pltpu.VMEM((NDEV, 2, KLOC), f32),
            pltpu.VMEM((2 * ROWS, DIM), bf16),
            pltpu.VMEM((NBUF, PCH, DIM), bf16),
            pltpu.VMEM((NBUF, 2 * ROWS, PCH), f32),
            dma(()), dma((5,)),
            dma((7,)), dma((7,)),
            dma((2, 4)), dma((2, 4)),
            dma((2, 3)), dma((2, 3)),
            dma((6, 7)), dma((6, 7)),
            dma((7,)), dma((7,)),
            dma((NBUF,)), dma((NBUF,)),
        ],
        compiler_params=pltpu.CompilerParams(
            collective_id=0, has_side_effects=True, vmem_limit_bytes=VM1 * 1024 * 1024),
        name="sinkhorn",
    )(z1, z2, m, c)


def grad_kernel(c_ref, w_ref, vecs_ref, own_ref, b_ref, p0_ref, p_hbm, stat_ref,
                q1_hbm, q2_hbm, dz1_ref, dz2_ref, dc_hbm, loss_ref,
                pbuf, qbuf, dcbuf, bcol, p_sem, q_sem, dc_sem):
    step = pl.program_id(0)
    last = KALL // TK - 1
    slot = lax.rem(step, 2)
    nck = TK // CK

    def p_load(st):
        sl = lax.rem(st, 2)
        return pltpu.make_async_copy(
            p_hbm.at[:, pl.ds(pl.multiple_of((st - 1) * TK, TK), TK)], pbuf.at[sl], p_sem.at[sl])

    def q_store(st, v):
        sl = lax.rem(st, 2)
        return pltpu.make_async_copy(
            qbuf.at[sl, v], (q1_hbm, q2_hbm)[v].at[:, pl.ds(pl.multiple_of(st * TK, TK), TK)],
            q_sem.at[sl, v])

    def dc_store(st, k):
        sl = lax.rem(st, 2)
        return pltpu.make_async_copy(
            dcbuf.at[sl, pl.ds(k * CK, CK)],
            dc_hbm.at[pl.ds(pl.multiple_of(st * TK + k * CK, CK), CK), :], dc_sem.at[sl, k])

    @pl.when(step == 0)
    def _():
        dz1_ref[...] = jnp.zeros_like(dz1_ref)
        dz2_ref[...] = jnp.zeros_like(dz2_ref)
        loss_ref[...] = stat_ref[0:1, :]
        pbuf[0] = p0_ref[...]

    @pl.when(step > 0)
    def _():
        p_load(step).wait()

    @pl.when(step < last)
    def _():
        p_load(step + 1).start()

    @pl.when(step >= 2)
    def _():
        for v in range(2):
            q_store(step - 2, v).wait()
        for k in range(nck):
            dc_store(step - 2, k).wait()

    g = stat_ref[1:2, 0:1]
    dz = jnp.zeros((2 * ROWS, DIM), jnp.float32)
    for t in range(TK // OS):
        cols = slice(t * OS, (t + 1) * OS)
        ps = [pbuf[slot, :ROWS, cols], pbuf[slot, ROWS:, cols]]
        qs = []
        for v in range(2):
            arow = jnp.concatenate([own_ref[v]] * (OS // 128), axis=1)
            q = (ps[v] * ps[v] * arow) * b_ref[step, v:v + 1, cols]
            qbuf[slot, v, :, cols] = q
            qs.append(q)
        gs = []
        for v in range(2):
            al = jnp.concatenate([own_ref[2 + v]] * (OS // 128), axis=1)
            gs.append((ps[v] * al - qs[1 - v] * g).astype(jnp.bfloat16))
        dz = dz + dot_nn(jnp.concatenate(gs, axis=0), c_ref[cols, :])
    dz1_ref[...] += dz[:ROWS]
    dz2_ref[...] += dz[ROWS:]

    for v in range(2):
        for t in range(TK // 128):
            blk = jnp.broadcast_to(b_ref[step, v:v + 1, t * 128:(t + 1) * 128], (128, 128))
            bcol[v, t * 128:(t + 1) * 128, :] = jnp.transpose(blk)

    tiles = (jnp.max(stat_ref[2:3, :]).astype(jnp.int32) + (ROWS - 1)) // ROWS

    def piece(t, idx):
        rows = slice(t * SUB, (t + 1) * SUB)
        w = w_ref[idx]
        vec = vecs_ref[idx]
        p = jnp.exp2(dot_nt(c_ref[rows, :], w) * C_EXP)
        p1, p2 = p[:, :ROWS], p[:, ROWS:]
        g1 = p1 * vec[0:1] - (p2 * p2 * bcol[1, rows, :]) * vec[3:4]
        g2 = p2 * vec[1:2] - (p1 * p1 * bcol[0, rows, :]) * vec[2:3]
        gg = jnp.concatenate([g1.astype(jnp.bfloat16), g2.astype(jnp.bfloat16)], axis=1)
        return dot_nn(gg, w)

    npc = TK // SUB

    def add_tiles(idx, n, flush):
        for t in range(npc):
            rows = slice(t * SUB, (t + 1) * SUB)
            dcbuf[slot, rows, :] += sum(piece(t, idx + i) for i in range(n))
            if flush and (t + 1) % (CK // SUB) == 0:
                dc_store(step, t // (CK // SUB)).start()

    for t in range(npc):
        dcbuf[slot, t * SUB:(t + 1) * SUB, :] = piece(t, 0) + piece(t, 1)
    for v in range(2):
        q_store(step, v).start()

    rest = tiles - 2
    fin = jnp.where(rest == 1, 1, jnp.where(rest % 2 == 1, 3, jnp.minimum(rest, 2)))

    def body(i, carry):
        add_tiles(2 + 2 * i, 2, False)
        return carry
    lax.fori_loop(0, (rest - fin) // 2, body, 0)

    for n in (1, 2, 3):
        @pl.when(fin == n)
        def _(n=n):
            add_tiles(tiles - n, n, True)

    @pl.when(fin == 0)
    def _():
        for k in range(nck):
            dc_store(step, k).start()

    @pl.when(step == last)
    def _():
        for st in (last - 1, last):
            for v in range(2):
                q_store(st, v).wait()
            for k in range(nck):
                dc_store(st, k).wait()


def grad_call(c, w, vecs, own, b, p0, p, stat):
    f32, bf16 = jnp.float32, jnp.bfloat16
    whole = lambda shape: pl.BlockSpec(shape, lambda i: (0,) * len(shape))
    hbm = pl.BlockSpec(memory_space=pl.ANY)
    vm = pl.BlockSpec(memory_space=pltpu.VMEM)
    dma = pltpu.SemaphoreType.DMA
    return pl.pallas_call(
        grad_kernel,
        grid=(KALL // TK,),
        in_specs=[
            pl.BlockSpec((TK, DIM), lambda i: (i, 0)),
            vm, vm, vm,
            vm,
            vm, hbm,
            vm,
        ],
        out_specs=[hbm, hbm, whole((ROWS, DIM)), whole((ROWS, DIM)), hbm, whole((1, 128))],
        out_shape=[
            jax.ShapeDtypeStruct((ROWS, KALL), f32),
            jax.ShapeDtypeStruct((ROWS, KALL), f32),
            jax.ShapeDtypeStruct((ROWS, DIM), f32),
            jax.ShapeDtypeStruct((ROWS, DIM), f32),
            jax.ShapeDtypeStruct((KALL, DIM), f32),
            jax.ShapeDtypeStruct((1, 128), f32),
        ],
        scratch_shapes=[
            pltpu.VMEM((2, 2 * ROWS, TK), f32),
            pltpu.VMEM((2, 2, ROWS, TK), f32),
            pltpu.VMEM((2, TK, DIM), f32),
            pltpu.VMEM((2, TK, 128), f32),
            dma((2,)), dma((2, 2)), dma((2, TK // CK)),
        ],
        compiler_params=pltpu.CompilerParams(vmem_limit_bytes=VM2 * 1024 * 1024),
        name="grads",
    )(c, w, vecs, own, b, p0, p, stat)


def solution(mesh):
    def local_step(view_one, view_two, protos, valid_mask):
        w, vecs, own, b, stat, p0, p = sink_call(
            view_one, view_two, valid_mask.reshape(1, ROWS), protos)
        q1, q2, dz1, dz2, dc, loss = grad_call(
            protos, w, vecs, own, b, p0, p, stat)
        return q1, q2, loss[0, 0], dz1, dz2, dc

    return jax.shard_map(
        local_step,
        mesh=mesh,
        in_specs=(P("data", None), P("data", None), P(None, None), P("data")),
        out_specs=(P("data", None), P("data", None), P(), P("data", None), P("data", None), P(None, None)),
        check_vma=False,
    )
```

```python
import functools

import jax
import jax.numpy as jnp
from jax import lax
from jax.experimental import pallas as pl
from jax.experimental.pallas import tpu as pltpu
from jax.sharding import PartitionSpec as P

SOFT_TEMP = 0.1
LOG2E = 1.4426950408889634
C_EXP = LOG2E / SOFT_TEMP
MESH = pl.DeviceIdType.MESH
NDEV = 8
ROWS = 128
NS = NDEV * ROWS
DIM = 256
KALL = 16384
KLOC = KALL // NDEV
GRP = 128
CH = 256
TK = 4096
SUB = 512
CK = 1024
OS = 256

PCH = 1024
NPC = KALL // PCH
NBUF = 4
SPLIT = (10, 12, 14, 16)

VM1 = 53
VM2 = 45
NT_DIMS = (((1,), (1,)), ((), ()))


def dot_nt(x, y):
    return lax.dot_general(x, y, NT_DIMS, preferred_element_type=jnp.float32)


def dot_nn(x, y):
    return jnp.dot(x, y, preferred_element_type=jnp.float32)


def sink_kernel(z1_hbm, z2_hbm, m_hbm, c_hbm,
                w_ref, vecs_ref, own_ref, b_out, stat_ref, p0_out, c0_out, p_hbm,
                z_all, m_all, cs, ps, zcs, s_ref, e_ref, bcol,
                ar1, ar1b, ar2, ar2b, ar3, ar3b, b_all, zz, cbuf, pbuf,
                c_sem, in_sem, m_send, m_recv, z_send, z_recv, f_send, f_recv,
                ar_send, ar_recv, b_send, b_recv, cb_sem, pb_sem):
    me = lax.axis_index("data")
    chip, core = me // 2, me % 2
    partner = 2 * chip + (1 - core)
    peers = [lax.rem(me + o, NDEV) for o in range(1, NDEV)]
    same = [2 * lax.rem(chip + d, 4) + core for d in range(1, 4)]

    barrier = pltpu.get_barrier_semaphore()
    for peer in peers:
        pl.semaphore_signal(barrier, inc=1, device_id=(peer,), device_id_type=MESH)

    loads = [pltpu.make_async_copy(src, dst, in_sem.at[i]) for i, (src, dst) in enumerate((
        (z1_hbm, z_all.at[0, me]), (z2_hbm, z_all.at[1, me]), (m_hbm, m_all.at[me]),
        (z1_hbm, zz.at[pl.ds(0, ROWS)]), (z2_hbm, zz.at[pl.ds(ROWS, ROWS)])))]
    for cp in loads:
        cp.start()

    def c_load(j):
        dst = c0_out.at[pl.ds(j * PCH, PCH), :] if j < TK // PCH else cbuf.at[j % NBUF]
        return pltpu.make_async_copy(c_hbm.at[pl.ds(j * PCH, PCH), :], dst, cb_sem.at[j % NBUF])

    def p_store(j):
        return pltpu.make_async_copy(
            pbuf.at[j % NBUF], p_hbm.at[:, pl.ds(j * PCH - TK, PCH)], pb_sem.at[j % NBUF])

    for j in range(NBUF):
        c_load(j).start()
    cslice = pltpu.make_async_copy(c_hbm.at[pl.ds(me * KLOC, KLOC), :], cs, c_sem)
    cslice.start()

    def own_scores(lo, hi):
        for j in range(lo, hi):
            c_load(j).wait()
            if j - NBUF >= TK // PCH:
                p_store(j - NBUF).wait()
            for t in range(PCH // 256):
                cols = slice(t * 256, (t + 1) * 256)
                rows = slice(j * PCH + t * 256, j * PCH + (t + 1) * 256)
                sc = dot_nt(zz[...], c0_out[rows, :] if j < TK // PCH else cbuf[j % NBUF, cols, :])
                if j < TK // PCH:
                    p0_out[:, j * PCH + t * 256:j * PCH + (t + 1) * 256] = jnp.exp2(sc * C_EXP)
                else:
                    pbuf[j % NBUF, :, cols] = jnp.exp2(sc * C_EXP)
            if j >= TK // PCH:
                p_store(j).start()
            if j + NBUF < NPC:
                c_load(j + NBUF).start()

    for cp in loads:
        cp.wait()
    pl.semaphore_wait(barrier, NDEV - 1)

    m_copies = []
    for o, peer in enumerate(peers):
        cp = pltpu.make_async_remote_copy(
            src_ref=m_all.at[me], dst_ref=m_all.at[me], send_sem=m_send.at[o],
            recv_sem=m_recv.at[o], device_id=(peer,), device_id_type=MESH)
        cp.start()
        m_copies.append(cp)
    z_copies = []
    for v in range(2):
        row = []
        for d, peer in enumerate(same + [partner]):
            cp = pltpu.make_async_remote_copy(
                src_ref=z_all.at[v, me], dst_ref=z_all.at[v, me], send_sem=z_send.at[v, d],
                recv_sem=z_recv.at[v, d], device_id=(peer,), device_id_type=MESH)
            cp.start()
            row.append(cp)
        z_copies.append(row)

    own_scores(0, SPLIT[0])
    for cp in m_copies:
        cp.wait_recv()
    mf = [jnp.broadcast_to(m_all[d].astype(jnp.float32), (8, ROWS)) for d in range(NDEV)]

    tri = (lax.broadcasted_iota(jnp.int32, (ROWS, ROWS), 0)
           < lax.broadcasted_iota(jnp.int32, (ROWS, ROWS), 1)).astype(jnp.bfloat16)
    base = jnp.zeros((8, 1), jnp.float32)
    pos_list = []
    for d in range(NDEV):
        md = mf[d]
        pre = dot_nn(md.astype(jnp.bfloat16), tri) + base
        pos_list.append(jnp.where(md > 0, pre, -1.0))
        base = base + jnp.sum(md, axis=1, keepdims=True)
    pos = jnp.concatenate(pos_list, axis=1)
    count = base
    mask = (lax.broadcasted_iota(jnp.int32, (8, NS), 1).astype(jnp.float32) < count)
    maskf = mask.astype(jnp.float32)
    for t in range(NS // 128):
        lo_col = t // 2 * 256
        idx = (lax.broadcasted_iota(jnp.int32, (128, NS - lo_col), 0) + t * 128).astype(jnp.float32)
        ps[t * 128:(t + 1) * 128, lo_col:] = (
            jnp.broadcast_to(pos[0:1, lo_col:], (128, NS - lo_col)) == idx).astype(jnp.bfloat16)

    def forward(v):
        out = []
        for d in range(3):
            z_copies[v][d].wait_recv()
            frm = 2 * lax.rem(chip + 3 - d, 4) + core
            cp = pltpu.make_async_remote_copy(
                src_ref=z_all.at[v, frm], dst_ref=z_all.at[v, frm], send_sem=f_send.at[v, d],
                recv_sem=f_recv.at[v, d], device_id=(partner,), device_id_type=MESH)
            cp.start()
            out.append(cp)
        return out

    def compact(v, fw):
        z_copies[v][3].wait_recv()
        for cp in fw:
            cp.wait_recv()
        zv = z_all[v].reshape(NS, DIM)
        for t in range(NS // 256):
            rows = slice(t * 256, (t + 1) * 256)
            zc = dot_nn(ps[rows, t * 256:], zv[t * 256:]).astype(jnp.bfloat16)
            zcs[v, rows, :] = zc
            w_ref[2 * t, v * ROWS:(v + 1) * ROWS, :] = zc[:ROWS]
            w_ref[2 * t + 1, v * ROWS:(v + 1) * ROWS, :] = zc[ROWS:]

    def exchange(idx, buf):
        copies = []
        for o, peer in enumerate(peers):
            cp = pltpu.make_async_remote_copy(
                src_ref=buf.at[me], dst_ref=buf.at[me], send_sem=ar_send.at[idx, o],
                recv_sem=ar_recv.at[idx, o], device_id=(peer,), device_id_type=MESH)
            cp.start()
            copies.append(cp)
        return copies

    def total(buf, copies):
        for cp in copies:
            cp.wait_recv()
        acc = buf[0]
        for d in range(1, NDEV):
            acc = acc + buf[d]
        return acc

    def rsum(x):
        return jnp.sum(x, axis=0, keepdims=True)

    m1 = maskf[0:1]

    def recip(r):
        return jnp.where(m1 > 0, 1.0 / jnp.where(m1 > 0, r, 1.0), 0.0)

    zero = jnp.zeros((8, NS), jnp.float32)

    def first_pass(v, lo, hi, carry):
        racc, lacc = carry

        def rows_part(i, racc):
            for g in range(CH // 8):
                rows = slice(i * CH + g * 8, i * CH + g * 8 + 8)
                b = jnp.concatenate([bcol[v, rows, :]] * (NS // 128), axis=1)
                racc = racc + e_ref[v, rows, :] * b
            return racc

        for i in range(lo, hi):
            off = i * CH
            s_ref[v, off:off + CH, :] = dot_nt(cs[off:off + CH, :], zcs[v])
            for g in range(CH // 8):
                rows = slice(off + g * 8, off + g * 8 + 8)
                p = jnp.exp2(s_ref[v, rows, :] * C_EXP)
                lacc = lacc + p
                e = p * p * maskf
                e_ref[v, rows, :] = e
                bcol[v, rows, :] = jnp.broadcast_to(1.0 / jnp.sum(e, axis=1, keepdims=True), (8, 128))
            if i > lo:
                racc = rows_part(i - 1, racc)
        return rows_part(hi - 1, racc), lacc

    def sweep(v, a, last):
        a8 = jnp.broadcast_to(a, (8, NS))

        def body(i, carry):
            carry = list(carry)
            off = pl.multiple_of(i * (GRP * 8), GRP * 8)
            for g in range(GRP):
                rows = pl.ds(off + g * 8, 8)
                e = e_ref[v, rows, :]
                b = 1.0 / jnp.sum(e * a8, axis=1, keepdims=True)
                eb = e * b
                carry[0] = carry[0] + eb
                if last:
                    bcol[v, rows, :] = jnp.broadcast_to(b, (8, 128))
                    carry[1] = carry[1] + eb * s_ref[1 - v, rows, :]
            return tuple(carry)
        return lax.fori_loop(0, KLOC // (GRP * 8), body, (zero,) * (2 if last else 1))

    half = KLOC // CH // 2
    fw1 = forward(0)
    own_scores(SPLIT[0], SPLIT[1])
    cslice.wait()
    compact(0, fw1)
    acc = first_pass(0, 0, half, (zero, zero))
    fw2 = forward(1)
    racc, lacc = first_pass(0, half, 2 * half, acc)
    ar1[me, 0:1, :] = rsum(racc)
    ar1[me, 1:2, :] = rsum(lacc)
    x1 = [exchange(0, ar1)]
    compact(1, fw2)
    racc, lacc = first_pass(1, 0, 2 * half, (zero, zero))
    ar1b[me, 0:1, :] = rsum(racc)
    ar1b[me, 1:2, :] = rsum(lacc)
    x1.append(exchange(1, ar1b))

    lse, x2 = [], []
    for v, (b1, b2) in enumerate(((ar1, ar2), (ar1b, ar2b))):
        if v == 1:
            own_scores(SPLIT[1], SPLIT[2])
        tot = total(b1, x1[v])
        lse.append(tot[1:2])
        r, = sweep(v, recip(tot[0:1]), False)
        b2[me] = rsum(r)
        x2.append(exchange(2 + v, b2))

    x3, b_copies = [], []
    eye = (lax.broadcasted_iota(jnp.int32, (128, 128), 0)
           == lax.broadcasted_iota(jnp.int32, (128, 128), 1))
    for v, (b2, b3) in enumerate(((ar2, ar3), (ar2b, ar3b))):
        if v == 1:
            own_scores(SPLIT[2], SPLIT[3])
        tot = total(b2, x2[v])
        r, tl = sweep(v, recip(tot), True)
        b3[me, 0:1, :] = rsum(r)
        b3[me, 1:2, :] = rsum(tl)
        x3.append(exchange(4 + v, b3))
        for t in range(KLOC // 128):
            blk = bcol[v, t * 128:(t + 1) * 128, :]
            b_all[me, v:v + 1, t * 128:(t + 1) * 128] = jnp.sum(
                jnp.where(eye, blk, 0.0), axis=0, keepdims=True)
    for o, peer in enumerate(peers):
        cp = pltpu.make_async_remote_copy(
            src_ref=b_all.at[me], dst_ref=b_all.at[me], send_sem=b_send.at[o],
            recv_sem=b_recv.at[o], device_id=(peer,), device_id_type=MESH)
        cp.start()
        b_copies.append(cp)

    cnt = count[0:1]
    g = 1.0 / (2.0 * SOFT_TEMP * cnt)
    alpha = [m1 * g / x for x in lse]
    stat_ref[1:2, :] = jnp.broadcast_to(g, (1, 128))
    stat_ref[2:3, :] = jnp.broadcast_to(cnt, (1, 128))
    before = jnp.zeros((1, 1), jnp.float32)
    for d in range(NDEV):
        before = before + jnp.where(d < me, 1.0, 0.0) * jnp.sum(mf[d][0:1], axis=1, keepdims=True)
    mine = jnp.broadcast_to(m_all[me].astype(jnp.float32), (8, ROWS))
    pre = dot_nn(mine.astype(jnp.bfloat16), tri)[0:1] + before
    pre = jnp.where(mine[0:1] > 0, pre, -1.0)
    pcol = jnp.sum(jnp.where(eye, jnp.broadcast_to(pre, (128, 128)), 0.0), axis=1, keepdims=True)
    lane = lax.broadcasted_iota(jnp.int32, (128, NS), 1).astype(jnp.float32)
    hit = lane == pcol

    def put(i, x, scale):
        col = jnp.sum(jnp.where(hit, jnp.broadcast_to(x, (128, NS)), 0.0), axis=1, keepdims=True)
        own_ref[i] = jnp.broadcast_to(col, (128, 128))
        y = x * scale
        for t in range(NDEV):
            j = (i + 2) % 4
            vecs_ref[t, j:j + 1, :] = y[:, t * 128:(t + 1) * 128]

    put(2, alpha[0], 1.0)
    put(3, alpha[1], 1.0)
    own_scores(SPLIT[3], NPC)

    tots = [total(ar3, x3[0])]
    a0 = recip(tots[0][0:1])
    put(0, a0, g)
    tots.append(total(ar3b, x3[1]))
    a1 = recip(tots[1][0:1])
    put(1, a1, g)
    inner = sum(a * (tots[v][1:2] * (1.0 / SOFT_TEMP)) - a * tots[v][0:1] * jnp.log(lse[1 - v])
                for v, a in enumerate((a0, a1)))
    loss = -jnp.sum(jnp.where(m1 > 0, inner, 0.0), axis=1, keepdims=True) / (2.0 * cnt)
    stat_ref[0:1, :] = jnp.broadcast_to(loss, (1, 128))

    for cp in b_copies:
        cp.wait_recv()
    for d in range(NDEV):
        lo_col = d * KLOC
        b_out[lo_col // TK, :, lo_col % TK:lo_col % TK + KLOC] = b_all[d]
    for j in range(NPC - NBUF, NPC):
        p_store(j).wait()
    for cp in m_copies + z_copies[0] + z_copies[1] + fw1 + fw2 + sum(x1 + x2 + x3, []) + b_copies:
        cp.wait_send()


def sink_call(z1, z2, m, c):
    f32, bf16 = jnp.float32, jnp.bfloat16
    vm = pl.BlockSpec(memory_space=pltpu.VMEM)
    hbm = pl.BlockSpec(memory_space=pltpu.HBM)
    dma = pltpu.SemaphoreType.DMA
    return pl.pallas_call(
        sink_kernel,
        in_specs=[hbm] * 4,
        out_specs=[vm] * 7 + [hbm],
        out_shape=[
            pltpu.VMEM((NDEV, 2 * ROWS, DIM), bf16),
            pltpu.VMEM((NDEV, 4, ROWS), f32),
            pltpu.VMEM((4, ROWS, 128), f32),
            pltpu.VMEM((KALL // TK, 2, TK), f32),
            pltpu.VMEM((3, 128), f32),
            pltpu.VMEM((2 * ROWS, TK), f32),
            pltpu.VMEM((TK, DIM), bf16),
            jax.ShapeDtypeStruct((2 * ROWS, KALL - TK), f32),
        ],
        scratch_shapes=[
            pltpu.VMEM((2, NDEV, ROWS, DIM), bf16),
            pltpu.VMEM((NDEV, 1, ROWS), jnp.int32),
            pltpu.VMEM((KLOC, DIM), bf16),
            pltpu.VMEM((NS, NS), bf16),
            pltpu.VMEM((2, NS, DIM), bf16),
            pltpu.VMEM((2, KLOC, NS), f32),
            pltpu.VMEM((2, KLOC, NS), f32),
            pltpu.VMEM((2, KLOC, 128), f32),
            pltpu.VMEM((NDEV, 2, NS), f32),
            pltpu.VMEM((NDEV, 2, NS), f32),
            pltpu.VMEM((NDEV, 1, NS), f32),
            pltpu.VMEM((NDEV, 1, NS), f32),
            pltpu.VMEM((NDEV, 2, NS), f32),
            pltpu.VMEM((NDEV, 2, NS), f32),
            pltpu.VMEM((NDEV, 2, KLOC), f32),
            pltpu.VMEM((2 * ROWS, DIM), bf16),
            pltpu.VMEM((NBUF, PCH, DIM), bf16),
            pltpu.VMEM((NBUF, 2 * ROWS, PCH), f32),
            dma(()), dma((5,)),
            dma((7,)), dma((7,)),
            dma((2, 4)), dma((2, 4)),
            dma((2, 3)), dma((2, 3)),
            dma((6, 7)), dma((6, 7)),
            dma((7,)), dma((7,)),
            dma((NBUF,)), dma((NBUF,)),
        ],
        compiler_params=pltpu.CompilerParams(
            collective_id=0, has_side_effects=True, vmem_limit_bytes=VM1 * 1024 * 1024),
        name="sinkhorn",
    )(z1, z2, m, c)


def grad_kernel(c0_ref, c_hbm, w_ref, vecs_ref, own_ref, b_ref, p0_ref, p_hbm, stat_ref,
                q1_hbm, q2_hbm, dz1_ref, dz2_ref, dc_hbm, loss_ref,
                cbuf, pbuf, qbuf, dcbuf, bcol, c_sem, p_sem, q_sem, dc_sem):
    step = pl.program_id(0)
    last = KALL // TK - 1
    slot = lax.rem(step, 2)
    nck = TK // CK

    def p_load(st):
        sl = lax.rem(st, 2)
        return pltpu.make_async_copy(
            p_hbm.at[:, pl.ds(pl.multiple_of((st - 1) * TK, TK), TK)], pbuf.at[sl], p_sem.at[sl])

    def c_load(st):
        sl = lax.rem(st, 2)
        return pltpu.make_async_copy(
            c_hbm.at[pl.ds(pl.multiple_of(st * TK, TK), TK), :], cbuf.at[sl], c_sem.at[sl])

    def q_store(st, v):
        sl = lax.rem(st, 2)
        return pltpu.make_async_copy(
            qbuf.at[sl, v], (q1_hbm, q2_hbm)[v].at[:, pl.ds(pl.multiple_of(st * TK, TK), TK)],
            q_sem.at[sl, v])

    def dc_store(st, k):
        sl = lax.rem(st, 2)
        return pltpu.make_async_copy(
            dcbuf.at[sl, pl.ds(k * CK, CK)],
            dc_hbm.at[pl.ds(pl.multiple_of(st * TK + k * CK, CK), CK), :], dc_sem.at[sl, k])

    @pl.when(step == 0)
    def _():
        dz1_ref[...] = jnp.zeros_like(dz1_ref)
        dz2_ref[...] = jnp.zeros_like(dz2_ref)
        loss_ref[...] = stat_ref[0:1, :]
        pbuf[0] = p0_ref[...]
        cbuf[0] = c0_ref[...]

    @pl.when(step > 0)
    def _():
        p_load(step).wait()
        c_load(step).wait()

    @pl.when(step < last)
    def _():
        p_load(step + 1).start()
        c_load(step + 1).start()

    @pl.when(step >= 2)
    def _():
        for v in range(2):
            q_store(step - 2, v).wait()
        for k in range(nck):
            dc_store(step - 2, k).wait()

    g = stat_ref[1:2, 0:1]
    dz = jnp.zeros((2 * ROWS, DIM), jnp.float32)
    for t in range(TK // OS):
        cols = slice(t * OS, (t + 1) * OS)
        ps = [pbuf[slot, :ROWS, cols], pbuf[slot, ROWS:, cols]]
        qs = []
        for v in range(2):
            arow = jnp.concatenate([own_ref[v]] * (OS // 128), axis=1)
            q = (ps[v] * ps[v] * arow) * b_ref[step, v:v + 1, cols]
            qbuf[slot, v, :, cols] = q
            qs.append(q)
        gs = []
        for v in range(2):
            al = jnp.concatenate([own_ref[2 + v]] * (OS // 128), axis=1)
            gs.append((ps[v] * al - qs[1 - v] * g).astype(jnp.bfloat16))
        dz = dz + dot_nn(jnp.concatenate(gs, axis=0), cbuf[slot, cols, :])
    dz1_ref[...] += dz[:ROWS]
    dz2_ref[...] += dz[ROWS:]

    for v in range(2):
        for t in range(TK // 128):
            blk = jnp.broadcast_to(b_ref[step, v:v + 1, t * 128:(t + 1) * 128], (128, 128))
            bcol[v, t * 128:(t + 1) * 128, :] = jnp.transpose(blk)

    tiles = (jnp.max(stat_ref[2:3, :]).astype(jnp.int32) + (ROWS - 1)) // ROWS

    def piece(t, idx):
        rows = slice(t * SUB, (t + 1) * SUB)
        w = w_ref[idx]
        vec = vecs_ref[idx]
        p = jnp.exp2(dot_nt(cbuf[slot, rows, :], w) * C_EXP)
        p1, p2 = p[:, :ROWS], p[:, ROWS:]
        g1 = p1 * vec[0:1] - (p2 * p2 * bcol[1, rows, :]) * vec[3:4]
        g2 = p2 * vec[1:2] - (p1 * p1 * bcol[0, rows, :]) * vec[2:3]
        gg = jnp.concatenate([g1.astype(jnp.bfloat16), g2.astype(jnp.bfloat16)], axis=1)
        return dot_nn(gg, w)

    npc = TK // SUB

    def add_tiles(idx, n, flush):
        for t in range(npc):
            rows = slice(t * SUB, (t + 1) * SUB)
            dcbuf[slot, rows, :] += sum(piece(t, idx + i) for i in range(n))
            if flush and (t + 1) % (CK // SUB) == 0:
                dc_store(step, t // (CK // SUB)).start()

    for t in range(npc):
        dcbuf[slot, t * SUB:(t + 1) * SUB, :] = piece(t, 0) + piece(t, 1)
    for v in range(2):
        q_store(step, v).start()

    rest = tiles - 2
    fin = jnp.where(rest == 1, 1, jnp.where(rest % 2 == 1, 3, jnp.minimum(rest, 2)))

    def body(i, carry):
        add_tiles(2 + 2 * i, 2, False)
        return carry
    lax.fori_loop(0, (rest - fin) // 2, body, 0)

    for n in (1, 2, 3):
        @pl.when(fin == n)
        def _(n=n):
            add_tiles(tiles - n, n, True)

    @pl.when(fin == 0)
    def _():
        for k in range(nck):
            dc_store(step, k).start()

    @pl.when(step == last)
    def _():
        for st in (last - 1, last):
            for v in range(2):
                q_store(st, v).wait()
            for k in range(nck):
                dc_store(st, k).wait()


def grad_call(c0, c, w, vecs, own, b, p0, p, stat):
    f32, bf16 = jnp.float32, jnp.bfloat16
    whole = lambda shape: pl.BlockSpec(shape, lambda i: (0,) * len(shape))
    hbm = pl.BlockSpec(memory_space=pl.ANY)
    vm = pl.BlockSpec(memory_space=pltpu.VMEM)
    dma = pltpu.SemaphoreType.DMA
    return pl.pallas_call(
        grad_kernel,
        grid=(KALL // TK,),
        in_specs=[
            vm, hbm,
            vm, vm, vm,
            vm,
            vm, hbm,
            vm,
        ],
        out_specs=[hbm, hbm, whole((ROWS, DIM)), whole((ROWS, DIM)), hbm, whole((1, 128))],
        out_shape=[
            jax.ShapeDtypeStruct((ROWS, KALL), f32),
            jax.ShapeDtypeStruct((ROWS, KALL), f32),
            jax.ShapeDtypeStruct((ROWS, DIM), f32),
            jax.ShapeDtypeStruct((ROWS, DIM), f32),
            jax.ShapeDtypeStruct((KALL, DIM), f32),
            jax.ShapeDtypeStruct((1, 128), f32),
        ],
        scratch_shapes=[
            pltpu.VMEM((2, TK, DIM), bf16),
            pltpu.VMEM((2, 2 * ROWS, TK), f32),
            pltpu.VMEM((2, 2, ROWS, TK), f32),
            pltpu.VMEM((2, TK, DIM), f32),
            pltpu.VMEM((2, TK, 128), f32),
            dma((2,)), dma((2,)), dma((2, 2)), dma((2, TK // CK)),
        ],
        compiler_params=pltpu.CompilerParams(vmem_limit_bytes=VM2 * 1024 * 1024),
        name="grads",
    )(c0, c, w, vecs, own, b, p0, p, stat)


def solution(mesh):
    def local_step(view_one, view_two, protos, valid_mask):
        w, vecs, own, b, stat, p0, c0, p = sink_call(
            view_one, view_two, valid_mask.reshape(1, ROWS), protos)
        q1, q2, dz1, dz2, dc, loss = grad_call(
            c0, protos, w, vecs, own, b, p0, p, stat)
        return q1, q2, loss[0, 0], dz1, dz2, dc

    return jax.shard_map(
        local_step,
        mesh=mesh,
        in_specs=(P("data", None), P("data", None), P(None, None), P("data")),
        out_specs=(P("data", None), P("data", None), P(), P("data", None), P("data", None), P(None, None)),
        check_vma=False,
    )
```

```python
import functools

import jax
import jax.numpy as jnp
from jax import lax
from jax.experimental import pallas as pl
from jax.experimental.pallas import tpu as pltpu
from jax.sharding import PartitionSpec as P

SOFT_TEMP = 0.1
LOG2E = 1.4426950408889634
C_EXP = LOG2E / SOFT_TEMP
MESH = pl.DeviceIdType.MESH
NDEV = 8
ROWS = 128
NS = NDEV * ROWS
DIM = 256
KALL = 16384
KLOC = KALL // NDEV
GRP = 128
CH = 512
TK = 4096
SUB = 512
CK = 1024
OS = 256

PCH = 1024
NPC = KALL // PCH
NBUF = 4
SPLIT = (10, 12, 14, 16)

VM1 = 53
VM2 = 45
NT_DIMS = (((1,), (1,)), ((), ()))


def dot_nt(x, y):
    return lax.dot_general(x, y, NT_DIMS, preferred_element_type=jnp.float32)


def dot_nn(x, y):
    return jnp.dot(x, y, preferred_element_type=jnp.float32)


def sink_kernel(z1_hbm, z2_hbm, m_hbm, c_hbm,
                w_ref, vecs_ref, own_ref, b_out, stat_ref, p0_out, c0_out, p_hbm,
                z_all, m_all, cs, ps, zcs, s_ref, e_ref, bcol,
                ar1, ar1b, ar2, ar2b, ar3, ar3b, b_all, zz, cbuf, pbuf,
                c_sem, in_sem, m_send, m_recv, z_send, z_recv, f_send, f_recv,
                ar_send, ar_recv, b_send, b_recv, cb_sem, pb_sem):
    me = lax.axis_index("data")
    chip, core = me // 2, me % 2
    partner = 2 * chip + (1 - core)
    peers = [lax.rem(me + o, NDEV) for o in range(1, NDEV)]
    same = [2 * lax.rem(chip + d, 4) + core for d in range(1, 4)]

    barrier = pltpu.get_barrier_semaphore()
    for peer in peers:
        pl.semaphore_signal(barrier, inc=1, device_id=(peer,), device_id_type=MESH)

    loads = [pltpu.make_async_copy(src, dst, in_sem.at[i]) for i, (src, dst) in enumerate((
        (z1_hbm, z_all.at[0, me]), (z2_hbm, z_all.at[1, me]), (m_hbm, m_all.at[me]),
        (z1_hbm, zz.at[pl.ds(0, ROWS)]), (z2_hbm, zz.at[pl.ds(ROWS, ROWS)])))]
    for cp in loads:
        cp.start()

    def c_load(j):
        dst = c0_out.at[pl.ds(j * PCH, PCH), :] if j < TK // PCH else cbuf.at[j % NBUF]
        return pltpu.make_async_copy(c_hbm.at[pl.ds(j * PCH, PCH), :], dst, cb_sem.at[j % NBUF])

    def p_store(j):
        return pltpu.make_async_copy(
            pbuf.at[j % NBUF], p_hbm.at[:, pl.ds(j * PCH - TK, PCH)], pb_sem.at[j % NBUF])

    for j in range(NBUF):
        c_load(j).start()
    cslice = pltpu.make_async_copy(c_hbm.at[pl.ds(me * KLOC, KLOC), :], cs, c_sem)
    cslice.start()

    def own_scores(lo, hi):
        for j in range(lo, hi):
            c_load(j).wait()
            if j - NBUF >= TK // PCH:
                p_store(j - NBUF).wait()
            for t in range(PCH // 256):
                cols = slice(t * 256, (t + 1) * 256)
                rows = slice(j * PCH + t * 256, j * PCH + (t + 1) * 256)
                sc = dot_nt(zz[...], c0_out[rows, :] if j < TK // PCH else cbuf[j % NBUF, cols, :])
                if j < TK // PCH:
                    p0_out[:, j * PCH + t * 256:j * PCH + (t + 1) * 256] = jnp.exp2(sc * C_EXP)
                else:
                    pbuf[j % NBUF, :, cols] = jnp.exp2(sc * C_EXP)
            if j >= TK // PCH:
                p_store(j).start()
            if j + NBUF < NPC:
                c_load(j + NBUF).start()

    for cp in loads:
        cp.wait()
    pl.semaphore_wait(barrier, NDEV - 1)

    m_copies = []
    for o, peer in enumerate(peers):
        cp = pltpu.make_async_remote_copy(
            src_ref=m_all.at[me], dst_ref=m_all.at[me], send_sem=m_send.at[o],
            recv_sem=m_recv.at[o], device_id=(peer,), device_id_type=MESH)
        cp.start()
        m_copies.append(cp)
    z_copies = []
    for v in range(2):
        row = []
        for d, peer in enumerate(same + [partner]):
            cp = pltpu.make_async_remote_copy(
                src_ref=z_all.at[v, me], dst_ref=z_all.at[v, me], send_sem=z_send.at[v, d],
                recv_sem=z_recv.at[v, d], device_id=(peer,), device_id_type=MESH)
            cp.start()
            row.append(cp)
        z_copies.append(row)

    own_scores(0, SPLIT[0])
    for cp in m_copies:
        cp.wait_recv()
    mf = [jnp.broadcast_to(m_all[d].astype(jnp.float32), (8, ROWS)) for d in range(NDEV)]

    tri = (lax.broadcasted_iota(jnp.int32, (ROWS, ROWS), 0)
           < lax.broadcasted_iota(jnp.int32, (ROWS, ROWS), 1)).astype(jnp.bfloat16)
    base = jnp.zeros((8, 1), jnp.float32)
    pos_list = []
    for d in range(NDEV):
        md = mf[d]
        pre = dot_nn(md.astype(jnp.bfloat16), tri) + base
        pos_list.append(jnp.where(md > 0, pre, -1.0))
        base = base + jnp.sum(md, axis=1, keepdims=True)
    pos = jnp.concatenate(pos_list, axis=1)
    count = base
    mask = (lax.broadcasted_iota(jnp.int32, (8, NS), 1).astype(jnp.float32) < count)
    maskf = mask.astype(jnp.float32)
    for t in range(NS // 128):
        lo_col = t // 2 * 256
        idx = (lax.broadcasted_iota(jnp.int32, (128, NS - lo_col), 0) + t * 128).astype(jnp.float32)
        ps[t * 128:(t + 1) * 128, lo_col:] = (
            jnp.broadcast_to(pos[0:1, lo_col:], (128, NS - lo_col)) == idx).astype(jnp.bfloat16)

    def forward(v):
        out = []
        for d in range(3):
            z_copies[v][d].wait_recv()
            frm = 2 * lax.rem(chip + 3 - d, 4) + core
            cp = pltpu.make_async_remote_copy(
                src_ref=z_all.at[v, frm], dst_ref=z_all.at[v, frm], send_sem=f_send.at[v, d],
                recv_sem=f_recv.at[v, d], device_id=(partner,), device_id_type=MESH)
            cp.start()
            out.append(cp)
        return out

    def compact(v, fw):
        z_copies[v][3].wait_recv()
        for cp in fw:
            cp.wait_recv()
        zv = z_all[v].reshape(NS, DIM)
        for t in range(NS // 256):
            rows = slice(t * 256, (t + 1) * 256)
            zc = dot_nn(ps[rows, t * 256:], zv[t * 256:]).astype(jnp.bfloat16)
            zcs[v, rows, :] = zc
            w_ref[2 * t, v * ROWS:(v + 1) * ROWS, :] = zc[:ROWS]
            w_ref[2 * t + 1, v * ROWS:(v + 1) * ROWS, :] = zc[ROWS:]

    def exchange(idx, buf):
        copies = []
        for o, peer in enumerate(peers):
            cp = pltpu.make_async_remote_copy(
                src_ref=buf.at[me], dst_ref=buf.at[me], send_sem=ar_send.at[idx, o],
                recv_sem=ar_recv.at[idx, o], device_id=(peer,), device_id_type=MESH)
            cp.start()
            copies.append(cp)
        return copies

    def total(buf, copies):
        for cp in copies:
            cp.wait_recv()
        acc = buf[0]
        for d in range(1, NDEV):
            acc = acc + buf[d]
        return acc

    def rsum(x):
        return jnp.sum(x, axis=0, keepdims=True)

    m1 = maskf[0:1]

    def recip(r):
        return jnp.where(m1 > 0, 1.0 / jnp.where(m1 > 0, r, 1.0), 0.0)

    zero = jnp.zeros((8, NS), jnp.float32)

    def first_pass(v, lo, hi, carry):
        racc, lacc = carry

        def rows_part(i, racc):
            for g in range(CH // 8):
                rows = slice(i * CH + g * 8, i * CH + g * 8 + 8)
                b = jnp.concatenate([bcol[v, rows, :]] * (NS // 128), axis=1)
                racc = racc + e_ref[v, rows, :] * b
            return racc

        for i in range(lo, hi):
            off = i * CH
            s_ref[v, off:off + CH, :] = dot_nt(cs[off:off + CH, :], zcs[v])
            for g in range(CH // 8):
                rows = slice(off + g * 8, off + g * 8 + 8)
                p = jnp.exp2(s_ref[v, rows, :] * C_EXP)
                lacc = lacc + p
                e = p * p * maskf
                e_ref[v, rows, :] = e
                bcol[v, rows, :] = jnp.broadcast_to(1.0 / jnp.sum(e, axis=1, keepdims=True), (8, 128))
            if i > lo:
                racc = rows_part(i - 1, racc)
        return rows_part(hi - 1, racc), lacc

    def sweep(v, a, last):
        a8 = jnp.broadcast_to(a, (8, NS))

        def body(i, carry):
            carry = list(carry)
            off = pl.multiple_of(i * (GRP * 8), GRP * 8)
            for g in range(GRP):
                rows = pl.ds(off + g * 8, 8)
                e = e_ref[v, rows, :]
                b = 1.0 / jnp.sum(e * a8, axis=1, keepdims=True)
                eb = e * b
                carry[0] = carry[0] + eb
                if last:
                    bcol[v, rows, :] = jnp.broadcast_to(b, (8, 128))
                    carry[1] = carry[1] + eb * s_ref[1 - v, rows, :]
            return tuple(carry)
        return lax.fori_loop(0, KLOC // (GRP * 8), body, (zero,) * (2 if last else 1))

    half = KLOC // CH // 2
    fw1 = forward(0)
    own_scores(SPLIT[0], SPLIT[1])
    cslice.wait()
    compact(0, fw1)
    acc = first_pass(0, 0, half, (zero, zero))
    fw2 = forward(1)
    racc, lacc = first_pass(0, half, 2 * half, acc)
    ar1[me, 0:1, :] = rsum(racc)
    ar1[me, 1:2, :] = rsum(lacc)
    x1 = [exchange(0, ar1)]
    compact(1, fw2)
    racc, lacc = first_pass(1, 0, 2 * half, (zero, zero))
    ar1b[me, 0:1, :] = rsum(racc)
    ar1b[me, 1:2, :] = rsum(lacc)
    x1.append(exchange(1, ar1b))

    lse, x2 = [], []
    for v, (b1, b2) in enumerate(((ar1, ar2), (ar1b, ar2b))):
        if v == 1:
            own_scores(SPLIT[1], SPLIT[2])
        tot = total(b1, x1[v])
        lse.append(tot[1:2])
        r, = sweep(v, recip(tot[0:1]), False)
        b2[me] = rsum(r)
        x2.append(exchange(2 + v, b2))

    x3, b_copies = [], []
    eye = (lax.broadcasted_iota(jnp.int32, (128, 128), 0)
           == lax.broadcasted_iota(jnp.int32, (128, 128), 1))
    for v, (b2, b3) in enumerate(((ar2, ar3), (ar2b, ar3b))):
        if v == 1:
            own_scores(SPLIT[2], SPLIT[3])
        tot = total(b2, x2[v])
        r, tl = sweep(v, recip(tot), True)
        b3[me, 0:1, :] = rsum(r)
        b3[me, 1:2, :] = rsum(tl)
        x3.append(exchange(4 + v, b3))
        for t in range(KLOC // 128):
            blk = bcol[v, t * 128:(t + 1) * 128, :]
            b_all[me, v:v + 1, t * 128:(t + 1) * 128] = jnp.sum(
                jnp.where(eye, blk, 0.0), axis=0, keepdims=True)
    for o, peer in enumerate(peers):
        cp = pltpu.make_async_remote_copy(
            src_ref=b_all.at[me], dst_ref=b_all.at[me], send_sem=b_send.at[o],
            recv_sem=b_recv.at[o], device_id=(peer,), device_id_type=MESH)
        cp.start()
        b_copies.append(cp)

    cnt = count[0:1]
    g = 1.0 / (2.0 * SOFT_TEMP * cnt)
    alpha = [m1 * g / x for x in lse]
    stat_ref[1:2, :] = jnp.broadcast_to(g, (1, 128))
    stat_ref[2:3, :] = jnp.broadcast_to(cnt, (1, 128))
    before = jnp.zeros((1, 1), jnp.float32)
    for d in range(NDEV):
        before = before + jnp.where(d < me, 1.0, 0.0) * jnp.sum(mf[d][0:1], axis=1, keepdims=True)
    mine = jnp.broadcast_to(m_all[me].astype(jnp.float32), (8, ROWS))
    pre = dot_nn(mine.astype(jnp.bfloat16), tri)[0:1] + before
    pre = jnp.where(mine[0:1] > 0, pre, -1.0)
    pcol = jnp.sum(jnp.where(eye, jnp.broadcast_to(pre, (128, 128)), 0.0), axis=1, keepdims=True)
    lane = lax.broadcasted_iota(jnp.int32, (128, NS), 1).astype(jnp.float32)
    hit = lane == pcol

    def put(i, x, scale):
        col = jnp.sum(jnp.where(hit, jnp.broadcast_to(x, (128, NS)), 0.0), axis=1, keepdims=True)
        own_ref[i] = jnp.broadcast_to(col, (128, 128))
        y = x * scale
        for t in range(NDEV):
            j = (i + 2) % 4
            vecs_ref[t, j:j + 1, :] = y[:, t * 128:(t + 1) * 128]

    put(2, alpha[0], 1.0)
    put(3, alpha[1], 1.0)
    own_scores(SPLIT[3], NPC)

    tots = [total(ar3, x3[0])]
    a0 = recip(tots[0][0:1])
    put(0, a0, g)
    tots.append(total(ar3b, x3[1]))
    a1 = recip(tots[1][0:1])
    put(1, a1, g)
    inner = sum(a * (tots[v][1:2] * (1.0 / SOFT_TEMP)) - a * tots[v][0:1] * jnp.log(lse[1 - v])
                for v, a in enumerate((a0, a1)))
    loss = -jnp.sum(jnp.where(m1 > 0, inner, 0.0), axis=1, keepdims=True) / (2.0 * cnt)
    stat_ref[0:1, :] = jnp.broadcast_to(loss, (1, 128))

    for cp in b_copies:
        cp.wait_recv()
    for d in range(NDEV):
        lo_col = d * KLOC
        b_out[lo_col // TK, :, lo_col % TK:lo_col % TK + KLOC] = b_all[d]
    for j in range(NPC - NBUF, NPC):
        p_store(j).wait()
    for cp in m_copies + z_copies[0] + z_copies[1] + fw1 + fw2 + sum(x1 + x2 + x3, []) + b_copies:
        cp.wait_send()


def sink_call(z1, z2, m, c):
    f32, bf16 = jnp.float32, jnp.bfloat16
    vm = pl.BlockSpec(memory_space=pltpu.VMEM)
    hbm = pl.BlockSpec(memory_space=pltpu.HBM)
    dma = pltpu.SemaphoreType.DMA
    return pl.pallas_call(
        sink_kernel,
        in_specs=[hbm] * 4,
        out_specs=[vm] * 7 + [hbm],
        out_shape=[
            pltpu.VMEM((NDEV, 2 * ROWS, DIM), bf16),
            pltpu.VMEM((NDEV, 4, ROWS), f32),
            pltpu.VMEM((4, ROWS, 128), f32),
            pltpu.VMEM((KALL // TK, 2, TK), f32),
            pltpu.VMEM((3, 128), f32),
            pltpu.VMEM((2 * ROWS, TK), f32),
            pltpu.VMEM((TK, DIM), bf16),
            jax.ShapeDtypeStruct((2 * ROWS, KALL - TK), f32),
        ],
        scratch_shapes=[
            pltpu.VMEM((2, NDEV, ROWS, DIM), bf16),
            pltpu.VMEM((NDEV, 1, ROWS), jnp.int32),
            pltpu.VMEM((KLOC, DIM), bf16),
            pltpu.VMEM((NS, NS), bf16),
            pltpu.VMEM((2, NS, DIM), bf16),
            pltpu.VMEM((2, KLOC, NS), f32),
            pltpu.VMEM((2, KLOC, NS), f32),
            pltpu.VMEM((2, KLOC, 128), f32),
            pltpu.VMEM((NDEV, 2, NS), f32),
            pltpu.VMEM((NDEV, 2, NS), f32),
            pltpu.VMEM((NDEV, 1, NS), f32),
            pltpu.VMEM((NDEV, 1, NS), f32),
            pltpu.VMEM((NDEV, 2, NS), f32),
            pltpu.VMEM((NDEV, 2, NS), f32),
            pltpu.VMEM((NDEV, 2, KLOC), f32),
            pltpu.VMEM((2 * ROWS, DIM), bf16),
            pltpu.VMEM((NBUF, PCH, DIM), bf16),
            pltpu.VMEM((NBUF, 2 * ROWS, PCH), f32),
            dma(()), dma((5,)),
            dma((7,)), dma((7,)),
            dma((2, 4)), dma((2, 4)),
            dma((2, 3)), dma((2, 3)),
            dma((6, 7)), dma((6, 7)),
            dma((7,)), dma((7,)),
            dma((NBUF,)), dma((NBUF,)),
        ],
        compiler_params=pltpu.CompilerParams(
            collective_id=0, has_side_effects=True, vmem_limit_bytes=VM1 * 1024 * 1024),
        name="sinkhorn",
    )(z1, z2, m, c)


def grad_kernel(c0_ref, c_hbm, w_ref, vecs_ref, own_ref, b_ref, p0_ref, p_hbm, stat_ref,
                q1_hbm, q2_hbm, dz1_ref, dz2_ref, dc_hbm, loss_ref,
                cbuf, pbuf, qbuf, dcbuf, bcol, c_sem, p_sem, q_sem, dc_sem):
    step = pl.program_id(0)
    last = KALL // TK - 1
    slot = lax.rem(step, 2)
    nck = TK // CK

    def p_load(st):
        sl = lax.rem(st, 2)
        return pltpu.make_async_copy(
            p_hbm.at[:, pl.ds(pl.multiple_of((st - 1) * TK, TK), TK)], pbuf.at[sl], p_sem.at[sl])

    def c_load(st):
        sl = lax.rem(st, 2)
        return pltpu.make_async_copy(
            c_hbm.at[pl.ds(pl.multiple_of(st * TK, TK), TK), :], cbuf.at[sl], c_sem.at[sl])

    def q_store(st, v):
        sl = lax.rem(st, 2)
        return pltpu.make_async_copy(
            qbuf.at[sl, v], (q1_hbm, q2_hbm)[v].at[:, pl.ds(pl.multiple_of(st * TK, TK), TK)],
            q_sem.at[sl, v])

    def dc_store(st, k):
        sl = lax.rem(st, 2)
        return pltpu.make_async_copy(
            dcbuf.at[sl, pl.ds(k * CK, CK)],
            dc_hbm.at[pl.ds(pl.multiple_of(st * TK + k * CK, CK), CK), :], dc_sem.at[sl, k])

    @pl.when(step == 0)
    def _():
        dz1_ref[...] = jnp.zeros_like(dz1_ref)
        dz2_ref[...] = jnp.zeros_like(dz2_ref)
        loss_ref[...] = stat_ref[0:1, :]
        pbuf[0] = p0_ref[...]
        cbuf[0] = c0_ref[...]

    @pl.when(step > 0)
    def _():
        p_load(step).wait()
        c_load(step).wait()

    @pl.when(step < last)
    def _():
        p_load(step + 1).start()
        c_load(step + 1).start()

    @pl.when(step >= 2)
    def _():
        for v in range(2):
            q_store(step - 2, v).wait()
        for k in range(nck):
            dc_store(step - 2, k).wait()

    g = stat_ref[1:2, 0:1]
    dz = jnp.zeros((2 * ROWS, DIM), jnp.float32)
    for t in range(TK // OS):
        cols = slice(t * OS, (t + 1) * OS)
        ps = [pbuf[slot, :ROWS, cols], pbuf[slot, ROWS:, cols]]
        qs = []
        for v in range(2):
            arow = jnp.concatenate([own_ref[v]] * (OS // 128), axis=1)
            q = (ps[v] * ps[v] * arow) * b_ref[step, v:v + 1, cols]
            qbuf[slot, v, :, cols] = q
            qs.append(q)
        gs = []
        for v in range(2):
            al = jnp.concatenate([own_ref[2 + v]] * (OS // 128), axis=1)
            gs.append((ps[v] * al - qs[1 - v] * g).astype(jnp.bfloat16))
        dz = dz + dot_nn(jnp.concatenate(gs, axis=0), cbuf[slot, cols, :])
    dz1_ref[...] += dz[:ROWS]
    dz2_ref[...] += dz[ROWS:]

    for v in range(2):
        for t in range(TK // 128):
            blk = jnp.broadcast_to(b_ref[step, v:v + 1, t * 128:(t + 1) * 128], (128, 128))
            bcol[v, t * 128:(t + 1) * 128, :] = jnp.transpose(blk)

    tiles = (jnp.max(stat_ref[2:3, :]).astype(jnp.int32) + (ROWS - 1)) // ROWS

    def piece(t, idx):
        rows = slice(t * SUB, (t + 1) * SUB)
        w = w_ref[idx]
        vec = vecs_ref[idx]
        p = jnp.exp2(dot_nt(cbuf[slot, rows, :], w) * C_EXP)
        p1, p2 = p[:, :ROWS], p[:, ROWS:]
        g1 = p1 * vec[0:1] - (p2 * p2 * bcol[1, rows, :]) * vec[3:4]
        g2 = p2 * vec[1:2] - (p1 * p1 * bcol[0, rows, :]) * vec[2:3]
        gg = jnp.concatenate([g1.astype(jnp.bfloat16), g2.astype(jnp.bfloat16)], axis=1)
        return dot_nn(gg, w)

    npc = TK // SUB

    def add_tiles(idx, n, flush):
        for t in range(npc):
            rows = slice(t * SUB, (t + 1) * SUB)
            dcbuf[slot, rows, :] += sum(piece(t, idx + i) for i in range(n))
            if flush and (t + 1) % (CK // SUB) == 0:
                dc_store(step, t // (CK // SUB)).start()

    for t in range(npc):
        dcbuf[slot, t * SUB:(t + 1) * SUB, :] = piece(t, 0) + piece(t, 1)
    for v in range(2):
        q_store(step, v).start()

    rest = tiles - 2
    fin = jnp.where(rest == 1, 1, jnp.where(rest % 2 == 1, 3, jnp.minimum(rest, 2)))

    def body(i, carry):
        add_tiles(2 + 2 * i, 2, False)
        return carry
    lax.fori_loop(0, (rest - fin) // 2, body, 0)

    for n in (1, 2, 3):
        @pl.when(fin == n)
        def _(n=n):
            add_tiles(tiles - n, n, True)

    @pl.when(fin == 0)
    def _():
        for k in range(nck):
            dc_store(step, k).start()

    @pl.when(step == last)
    def _():
        for st in (last - 1, last):
            for v in range(2):
                q_store(st, v).wait()
            for k in range(nck):
                dc_store(st, k).wait()


def grad_call(c0, c, w, vecs, own, b, p0, p, stat):
    f32, bf16 = jnp.float32, jnp.bfloat16
    whole = lambda shape: pl.BlockSpec(shape, lambda i: (0,) * len(shape))
    hbm = pl.BlockSpec(memory_space=pl.ANY)
    vm = pl.BlockSpec(memory_space=pltpu.VMEM)
    dma = pltpu.SemaphoreType.DMA
    return pl.pallas_call(
        grad_kernel,
        grid=(KALL // TK,),
        in_specs=[
            vm, hbm,
            vm, vm, vm,
            vm,
            vm, hbm,
            vm,
        ],
        out_specs=[hbm, hbm, whole((ROWS, DIM)), whole((ROWS, DIM)), hbm, whole((1, 128))],
        out_shape=[
            jax.ShapeDtypeStruct((ROWS, KALL), f32),
            jax.ShapeDtypeStruct((ROWS, KALL), f32),
            jax.ShapeDtypeStruct((ROWS, DIM), f32),
            jax.ShapeDtypeStruct((ROWS, DIM), f32),
            jax.ShapeDtypeStruct((KALL, DIM), f32),
            jax.ShapeDtypeStruct((1, 128), f32),
        ],
        scratch_shapes=[
            pltpu.VMEM((2, TK, DIM), bf16),
            pltpu.VMEM((2, 2 * ROWS, TK), f32),
            pltpu.VMEM((2, 2, ROWS, TK), f32),
            pltpu.VMEM((2, TK, DIM), f32),
            pltpu.VMEM((2, TK, 128), f32),
            dma((2,)), dma((2,)), dma((2, 2)), dma((2, TK // CK)),
        ],
        compiler_params=pltpu.CompilerParams(vmem_limit_bytes=VM2 * 1024 * 1024),
        name="grads",
    )(c0, c, w, vecs, own, b, p0, p, stat)


def solution(mesh):
    def local_step(view_one, view_two, protos, valid_mask):
        w, vecs, own, b, stat, p0, c0, p = sink_call(
            view_one, view_two, valid_mask.reshape(1, ROWS), protos)
        q1, q2, dz1, dz2, dc, loss = grad_call(
            c0, protos, w, vecs, own, b, p0, p, stat)
        return q1, q2, loss[0, 0], dz1, dz2, dc

    return jax.shard_map(
        local_step,
        mesh=mesh,
        in_specs=(P("data", None), P("data", None), P(None, None), P("data")),
        out_specs=(P("data", None), P("data", None), P(), P("data", None), P("data", None), P(None, None)),
        check_vma=False,
    )
```
